128 devices in a mesh: parts: 128 (over y, x, z, core).
Axes of the slice: x: 4, y: 4, z: 4, core: 2. Of those that a mesh axis runs over, the one named last changes fastest.
Arguments:
- rhs: float32 [216, 65536], P(None, 'parts'), may hold values from -60 to 90
- start: float32 [216, 65536], P(None, 'parts'), may hold values from -3.75 to 5.625
- spectrum_top: float32 [1], replicated, may hold values from 10 to 20
- elem_code: int32 [65536], P('parts'), may hold values from 0 to 2, as said below
- rec_elem: int32 [393216], P('parts'), may hold values from 0 to 511, as said below
- rec_dir: int32 [393216], P('parts'), may hold values from 0 to 5
- rec_sub: int32 [393216], P('parts'), may hold values from 0 to 5, as said below
- rec_peer: int32 [393216], P('parts'), may hold values from -1 to 127, as said below
- rec_index: int32 [393216], P('parts'), may hold values from 0 to 3071, as said below
- send_rec: int32 [4194304], P('parts'), may hold values from 0 to 3071, as said below
Outputs:
- solution: float32 [216, 65536], P(None, 'parts')
- norms: float32 [3, 2], replicated
The draws below stay inside these ranges and needn't reach their ends.
Inputs may be any that keep to these rules, and one draw needn't show every extreme that they name: `elem_code`: 0 marks an empty slot, 1 a fine element, 2 a coarse element; a device's live slots come first. `rec_elem`: always a live element of the record's device. `rec_sub`: 0 to 3: a quarter of a coarse face facing a fine element; 4: the whole face; 5: an unused slot, which comes after the device's used records. `rec_peer`: -1 at the channel's ends and on unused slots. A partner is never more than 7 devices away; its face has the opposite direction, and the partner's partner is the record itself. `rec_index`: A record index on the same device, or a slot of the partner device's send list to this device. `send_rec`: entries of slots that no record names are arbitrary. At most 256 slots are named from one device to another, and some pair of devices uses all 256.
All inputs are finite; a program needn't handle non-finite values.
Results may differ from the reference program's by a relative error of at most 0.0003.
Values sent between devices are 32-bit elements; how exact they have to be, the bound alone decides.
No kernel may reach another device: no remote copies, remote signals or barrier semaphores. Data moves between devices by JAX's collectives and lax.ppermute only.
A program may use at most 128 MiB of HBM per device.

```python
import math
import jax
import jax.numpy as jnp
import numpy as np
from jax import lax

NODES = 216
US = 8
LX_DEV = 1
LD = 4
ITERS = 3
ELEMS = 65536
N_PARTS = 128


def spread_bits(number):
    result = jnp.zeros_like(number)
    for bit_index in range(4):
        result = result | (number >> bit_index & 1) << 2 * bit_index
    return result


def gather_bits(number):
    result = jnp.zeros_like(number)
    for bit_index in range(4):
        result = result | (number >> 2 * bit_index & 1) << bit_index
    return result


def shuffle_group(sub_key):
    return jax.random.permutation(sub_key, LD).astype(jnp.int32)


def mesh_layout(key):
    units_dev = LX_DEV * US * US
    unit_total = N_PARTS * units_dev
    elem_dev = 8 * units_dev
    rec_dev = 48 * units_dev
    capacity = max(4 * US * US, 8 * LX_DEV * US)
    cross_span = 2 * US
    group_count = N_PARTS // LD
    length_span = group_count * LX_DEV
    far_reach = 2 * LD - 1
    group_keys = jax.random.split(jax.random.fold_in(key, 11), group_count)
    place_of = jax.vmap(shuffle_group)(group_keys)
    quadrant_of = jnp.argsort(place_of, axis=1).astype(jnp.int32)
    unit_id = jnp.arange(unit_total, dtype=jnp.int32)
    device_of = unit_id // units_dev
    coin_flip = jax.random.randint(jax.random.fold_in(key, 7), (unit_total,), 0, 5)
    refined = (coin_flip < 2) | (device_of < 2 * LD)
    local_unit = unit_id % units_dev
    morton = local_unit % (US * US)
    own_quadrant = quadrant_of[device_of // LD, device_of % LD]
    coord_x = device_of // LD * LX_DEV + local_unit // (US * US)
    coord_y = own_quadrant % 2 * US + gather_bits(morton)
    coord_z = own_quadrant // 2 * US + gather_bits(morton >> 1)

    def unit_at(pos_x, pos_y, pos_z):
        group_index = pos_x // LX_DEV
        quadrant = pos_y // US + 2 * (pos_z // US)
        device = group_index * LD + place_of[group_index, quadrant]
        inner_index = spread_bits(pos_y % US) | spread_bits(pos_z % US) << 1
        return device * units_dev + pos_x % LX_DEV * US * US + inner_index
    child_index = jnp.arange(8, dtype=jnp.int32)[None, :, None]
    direction = jnp.arange(6, dtype=jnp.int32)[None, None, :]
    axis_index = direction // 2
    face_side = direction % 2
    bit_x = child_index & 1
    bit_y = child_index >> 1 & 1
    bit_z = child_index >> 2 & 1
    bit_axis = jnp.where(axis_index == 0, bit_x, jnp.where(axis_index == 1, bit_y, bit_z))
    first_bit = jnp.where(axis_index == 0, bit_y, bit_x)
    second_bit = jnp.where(axis_index == 2, bit_y, bit_z)
    step_sign = 2 * face_side - 1
    near_x = coord_x[:, None, None] + step_sign * (axis_index == 0).astype(jnp.int32)
    near_y = (coord_y[:, None, None] + step_sign * (axis_index == 1).astype(jnp.int32)) % cross_span
    near_z = (coord_z[:, None, None] + step_sign * (axis_index == 2).astype(jnp.int32)) % cross_span
    outside = (near_x < 0) | (near_x >= length_span)
    near_unit = unit_at(jnp.clip(near_x, 0, length_span - 1), near_y, near_z)
    near_refined = refined[near_unit]
    own_refined = refined[:, None, None]
    internal = own_refined & (bit_axis != face_side)
    flip_child = child_index ^ 1 << axis_index
    coarse_slot = first_bit + 2 * second_bit
    facing = 1 - face_side
    low_bit = child_index & 1
    high_bit = child_index >> 1 & 1
    facing_child = jnp.where(axis_index == 0, facing + 2 * low_bit + 4 * high_bit, jnp.where(axis_index == 1, low_bit + 2 * facing + 4 * high_bit, low_bit + 2 * high_bit + 4 * facing))
    shape_all = (unit_total, 8, 6)
    partner_unit = jnp.where(internal, unit_id[:, None, None], near_unit)
    partner_child = jnp.where(own_refined, jnp.where(internal | near_refined, flip_child, coarse_slot), jnp.where(near_refined, facing_child, 0))
    boundary = jnp.logical_not(internal) & outside
    valid_mask = jnp.where(own_refined, True, (child_index == 0) | (child_index < 4) & near_refined & jnp.logical_not(outside))
    sub_code = jnp.where(own_refined | outside | jnp.logical_not(near_refined), 4, child_index)
    unit_size = jnp.where(refined, 8, 1).astype(jnp.int32)
    start_all = jnp.cumsum(unit_size) - unit_size
    elem_offset = start_all - start_all[device_of * units_dev]
    elem_local = elem_offset[:, None, None] + jnp.where(own_refined, child_index, 0)
    child_row = jnp.arange(8, dtype=jnp.int32)[None, :]
    elem_slot = device_of[:, None] * elem_dev + elem_offset[:, None] + child_row
    keep_slot = refined[:, None] | (child_row == 0)
    elem_value = jnp.broadcast_to(jnp.where(refined, 1, 2).astype(jnp.int32)[:, None], (unit_total, 8))
    elem_code = jnp.zeros((N_PARTS * elem_dev,), jnp.int32).at[jnp.where(keep_slot, elem_slot, N_PARTS * elem_dev).reshape(-1)].set(elem_value.reshape(-1), mode='drop')
    valid_flat = jnp.broadcast_to(valid_mask, shape_all).reshape(-1)
    bound_flat = jnp.broadcast_to(boundary, shape_all).reshape(-1)
    valid_count = valid_flat.astype(jnp.int32)
    before = jnp.cumsum(valid_count) - valid_count
    cand_total = unit_total * 48
    cand_device = jnp.arange(cand_total, dtype=jnp.int32) // rec_dev
    local_rec = before - before[cand_device * rec_dev]
    partner_cand = (jnp.broadcast_to(partner_unit, shape_all) * 48 + jnp.broadcast_to(partner_child, shape_all) * 6 + jnp.broadcast_to(direction ^ 1, shape_all)).reshape(-1)
    partner_cand = jnp.where(bound_flat, 0, partner_cand)
    partner_device = partner_cand // rec_dev
    remote = valid_flat & jnp.logical_not(bound_flat) & (partner_device != cand_device)
    offset = jnp.clip(partner_device - cand_device + far_reach, 0, 2 * far_reach)
    onehot = ((offset[:, None] == jnp.arange(2 * far_reach + 1, dtype=jnp.int32)[None, :]) & remote[:, None]).astype(jnp.int32)
    running = jnp.cumsum(onehot, axis=0) - onehot
    running = running - running[cand_device * rec_dev]
    send_slot = jnp.take_along_axis(running, offset[:, None], axis=1)[:, 0]
    target = jnp.where(valid_flat, cand_device * rec_dev + local_rec, N_PARTS * rec_dev)
    slot_total = N_PARTS * rec_dev
    rec_elem = jnp.zeros((slot_total,), jnp.int32).at[target].set(jnp.broadcast_to(elem_local, shape_all).reshape(-1), mode='drop')
    rec_dir = jnp.zeros((slot_total,), jnp.int32).at[target].set(jnp.broadcast_to(direction, shape_all).reshape(-1), mode='drop')
    rec_sub = jnp.full((slot_total,), 5, jnp.int32).at[target].set(jnp.broadcast_to(sub_code, shape_all).reshape(-1), mode='drop')
    rec_peer = jnp.full((slot_total,), -1, jnp.int32).at[target].set(jnp.where(bound_flat, -1, partner_device), mode='drop')
    index_value = jnp.where(bound_flat, 0, jnp.where(remote, send_slot[partner_cand], local_rec[partner_cand]))
    rec_index = jnp.zeros((slot_total,), jnp.int32).at[target].set(index_value, mode='drop')
    link_total = N_PARTS * N_PARTS * capacity
    link_slot = jnp.where(remote, (cand_device * N_PARTS + partner_device) * capacity + send_slot, link_total)
    send_rec = jnp.zeros((link_total,), jnp.int32).at[link_slot].set(local_rec, mode='drop')
    return (elem_code, rec_elem, rec_dir, rec_sub, rec_peer, rec_index, send_rec)


def draw_elem_code(key, part):
    return mesh_layout(jax.random.fold_in(key, 3))[0]


def draw_rec_elem(key, part):
    return mesh_layout(jax.random.fold_in(key, 3))[1]


def draw_rec_dir(key, part):
    return mesh_layout(jax.random.fold_in(key, 3))[2]


def draw_rec_sub(key, part):
    return mesh_layout(jax.random.fold_in(key, 3))[3]


def draw_rec_peer(key, part):
    return mesh_layout(jax.random.fold_in(key, 3))[4]


def draw_rec_index(key, part):
    return mesh_layout(jax.random.fold_in(key, 3))[5]


def draw_send_rec(key, part):
    return mesh_layout(jax.random.fold_in(key, 3))[6]


def field_draw(key, base_scale):
    column = jnp.arange(ELEMS, dtype=jnp.float32) / ELEMS
    rough = jnp.clip(jax.random.normal(key, (NODES, ELEMS), jnp.float32), -5.0, 5.0)
    return base_scale * (1.0 + 2.0 * column)[None, :] * rough


def draw_rhs(key, part):
    return field_draw(jax.random.fold_in(key, 21), 4.0)


def draw_start(key, part):
    return field_draw(jax.random.fold_in(key, 22), 0.25)


def setup_inputs(seed: int = 0) -> dict:
    splits = jax.random.split(jax.random.key(seed), 11)
    return {
        "rhs": draw_rhs(jax.random.fold_in(splits[10], 71), 0),
        "start": draw_start(jax.random.fold_in(splits[10], 71), 0),
        "spectrum_top": jnp.clip(jax.random.uniform(splits[2], (1,), jnp.float32, 10.0, 20.0), 10.0, 20.0),
        "elem_code": draw_elem_code(jax.random.fold_in(splits[10], 71), 0),
        "rec_elem": draw_rec_elem(jax.random.fold_in(splits[10], 71), 0),
        "rec_dir": draw_rec_dir(jax.random.fold_in(splits[10], 71), 0),
        "rec_sub": draw_rec_sub(jax.random.fold_in(splits[10], 71), 0),
        "rec_peer": draw_rec_peer(jax.random.fold_in(splits[10], 71), 0),
        "rec_index": draw_rec_index(jax.random.fold_in(splits[10], 71), 0),
        "send_rec": draw_send_rec(jax.random.fold_in(splits[10], 71), 0),
    }


PENALTY = 36.0
BOTTOM_RATIO = 8.0
HIGHEST = lax.Precision.HIGHEST

def lobatto_tables():
    root_seven = math.sqrt(7.0)
    inner_root = math.sqrt(1.0 / 3.0 - 2.0 * root_seven / 21.0)
    outer_root = math.sqrt(1.0 / 3.0 + 2.0 * root_seven / 21.0)
    points = (np.array([-1.0, -outer_root, -inner_root, inner_root, outer_root, 1.0]) + 1.0) / 2.0
    weights = np.array([1.0 / 15.0, (14.0 - root_seven) / 30.0, (14.0 + root_seven) / 30.0, (14.0 + root_seven) / 30.0, (14.0 - root_seven) / 30.0, 1.0 / 15.0]) / 2.0
    barycentric = np.array([1.0 / np.prod([points[j] - points[k] for k in range(6) if k != j]) for j in range(6)])
    derivative = np.zeros((6, 6))
    for i in range(6):
        for j in range(6):
            if i != j:
                derivative[i, j] = barycentric[j] / barycentric[i] / (points[i] - points[j])
        derivative[i, i] = -np.sum(derivative[i])
    halves = np.zeros((2, 6, 6))
    for which_half in range(2):
        targets = (points + which_half) / 2.0
        for i in range(6):
            for j in range(6):
                halves[which_half, i, j] = np.prod([(targets[i] - points[k]) / (points[j] - points[k]) for k in range(6) if k != j])
    column_sums = np.sum(derivative * derivative * weights[:, None], axis=0)
    stiff_diag = column_sums[:, None, None] * weights[None, :, None] * weights[None, None, :] + weights[:, None, None] * column_sums[None, :, None] * weights[None, None, :] + weights[:, None, None] * weights[None, :, None] * column_sums[None, None, :]
    return (weights, derivative, halves, stiff_diag.reshape(216))

def float_tables():
    weights, derivative, halves, stiff_diag = lobatto_tables()
    return (jnp.asarray(weights, dtype=jnp.float32), jnp.asarray(derivative, dtype=jnp.float32), jnp.asarray(halves, dtype=jnp.float32), jnp.asarray(stiff_diag, dtype=jnp.float32))

def face_traces(nodal_field, inv_size, derivative):
    values = []
    normals = []
    for direction in range(6):
        axis_index = direction // 2
        layer_index = 5 * (direction % 2)
        orientation = 2.0 * (direction % 2) - 1.0
        slope_row = derivative[layer_index]
        if axis_index == 0:
            face_value = nodal_field[layer_index]
            normal = jnp.einsum('m,mjke->jke', slope_row, nodal_field, precision=HIGHEST)
        elif axis_index == 1:
            face_value = nodal_field[:, layer_index]
            normal = jnp.einsum('m,imke->ike', slope_row, nodal_field, precision=HIGHEST)
        else:
            face_value = nodal_field[:, :, layer_index]
            normal = jnp.einsum('m,ijme->ije', slope_row, nodal_field, precision=HIGHEST)
        values.append(face_value.reshape(36, -1))
        normals.append((normal * (orientation * inv_size)).reshape(36, -1))
    return (jnp.concatenate(values, axis=1), jnp.concatenate(normals, axis=1))

def lift_faces(face_value, face_slope, inv_size, derivative, elem_count):
    result = jnp.zeros((6, 6, 6, elem_count), jnp.float32)
    for direction in range(6):
        axis_index = direction // 2
        layer_index = 5 * (direction % 2)
        orientation = 2.0 * (direction % 2) - 1.0
        slope_row = derivative[layer_index]
        part_value = face_value[:, direction * elem_count:(direction + 1) * elem_count].reshape(6, 6, elem_count)
        part_slope = face_slope[:, direction * elem_count:(direction + 1) * elem_count].reshape(6, 6, elem_count)
        part_slope = part_slope * (orientation * inv_size)
        if axis_index == 0:
            result = result.at[layer_index].add(part_value)
            result = result + jnp.einsum('m,jke->mjke', slope_row, part_slope, precision=HIGHEST)
        elif axis_index == 1:
            result = result.at[:, layer_index].add(part_value)
            result = result + jnp.einsum('m,ike->imke', slope_row, part_slope, precision=HIGHEST)
        else:
            result = result.at[:, :, layer_index].add(part_value)
            result = result + jnp.einsum('m,ije->ijme', slope_row, part_slope, precision=HIGHEST)
    return result

def volume_term(nodal_field, elem_size, weight_cube, derivative):
    cube_scale = weight_cube[:, :, :, None] * elem_size
    grad_x = jnp.einsum('im,mjke->ijke', derivative, nodal_field, precision=HIGHEST) * cube_scale
    grad_y = jnp.einsum('jm,imke->ijke', derivative, nodal_field, precision=HIGHEST) * cube_scale
    grad_z = jnp.einsum('km,ijme->ijke', derivative, nodal_field, precision=HIGHEST) * cube_scale
    result = jnp.einsum('mi,mjke->ijke', derivative, grad_x, precision=HIGHEST)
    result = result + jnp.einsum('mj,imke->ijke', derivative, grad_y, precision=HIGHEST)
    return result + jnp.einsum('mk,ijme->ijke', derivative, grad_z, precision=HIGHEST)

def onto_mortar(face_nodes, rec_sub, halves):
    whole_face = rec_sub >= 4
    first_bit = rec_sub % 2
    second_bit = rec_sub // 2 % 2
    lower_half = jnp.einsum('ij,jkr->ikr', halves[0], face_nodes, precision=HIGHEST)
    upper_half = jnp.einsum('ij,jkr->ikr', halves[1], face_nodes, precision=HIGHEST)
    face_nodes = jnp.where(whole_face, face_nodes, jnp.where(first_bit == 0, lower_half, upper_half))
    lower_half = jnp.einsum('kj,ijr->ikr', halves[0], face_nodes, precision=HIGHEST)
    upper_half = jnp.einsum('kj,ijr->ikr', halves[1], face_nodes, precision=HIGHEST)
    return jnp.where(whole_face, face_nodes, jnp.where(second_bit == 0, lower_half, upper_half))

def off_mortar(face_nodes, rec_sub, halves):
    whole_face = rec_sub >= 4
    first_bit = rec_sub % 2
    second_bit = rec_sub // 2 % 2
    lower_half = jnp.einsum('jk,ijr->ikr', halves[0], face_nodes, precision=HIGHEST)
    upper_half = jnp.einsum('jk,ijr->ikr', halves[1], face_nodes, precision=HIGHEST)
    face_nodes = jnp.where(whole_face, face_nodes, jnp.where(second_bit == 0, lower_half, upper_half))
    lower_half = jnp.einsum('ji,jkr->ikr', halves[0], face_nodes, precision=HIGHEST)
    upper_half = jnp.einsum('ji,jkr->ikr', halves[1], face_nodes, precision=HIGHEST)
    return jnp.where(whole_face, face_nodes, jnp.where(first_bit == 0, lower_half, upper_half))

def mortar_traces(face_value, face_slope, rec_col, rec_sub, halves):
    record_total = rec_col.shape[0]
    value_part = onto_mortar(face_value[:, rec_col].reshape(6, 6, record_total), rec_sub, halves)
    slope_part = onto_mortar(face_slope[:, rec_col].reshape(6, 6, record_total), rec_sub, halves)
    return jnp.concatenate([value_part.reshape(36, record_total), slope_part.reshape(36, record_total)], axis=0)

def mortar_terms(own_traces, partner, is_bound, mortar_size, live_rec, face_weight):
    own_value = own_traces[:36]
    own_slope = own_traces[36:]
    part_value = jnp.where(is_bound, 0.0, partner[:36])
    part_slope = jnp.where(is_bound, -own_slope, partner[36:])
    jump_value = own_value - part_value
    flux_value = 0.5 * (own_slope - part_slope)
    adjoint = jnp.where(is_bound, 1.0, 0.5)
    area_scale = mortar_size * mortar_size
    weight_live = face_weight[:, None] * live_rec
    term_value = weight_live * (PENALTY * mortar_size * jump_value - area_scale * flux_value)
    term_slope = -weight_live * adjoint * area_scale * jump_value
    return (term_value, term_slope)

def scatter_faces(term_value, term_slope, rec_col, rec_sub, halves, column_count):
    record_total = rec_col.shape[0]
    back_value = off_mortar(term_value.reshape(6, 6, record_total), rec_sub, halves).reshape(36, record_total)
    back_slope = off_mortar(term_slope.reshape(6, 6, record_total), rec_sub, halves).reshape(36, record_total)
    face_value = jnp.zeros((36, column_count), jnp.float32).at[:, rec_col].add(back_value)
    face_slope = jnp.zeros((36, column_count), jnp.float32).at[:, rec_col].add(back_slope)
    return (face_value, face_slope)

def reference(rhs, start, spectrum_top, elem_code, rec_elem, rec_dir, rec_sub, rec_peer, rec_index, send_rec):
    weights, derivative, halves, stiff_diag = float_tables()
    elem_total = rhs.shape[1]
    record_total = rec_elem.shape[0]
    elem_dev = elem_total // N_PARTS
    rec_dev = record_total // N_PARTS
    capacity = send_rec.shape[0] // (N_PARTS * N_PARTS)
    owner_device = jnp.arange(record_total, dtype=jnp.int32) // rec_dev
    global_elem = owner_device * elem_dev + rec_elem
    rec_col = rec_dir * elem_total + global_elem
    code_float = elem_code.astype(jnp.float32)
    elem_size = 0.5 * code_float
    inv_size = jnp.where(elem_code > 0, 2.0 / jnp.maximum(code_float, 1.0), 0.0)
    live_elem = elem_code > 0
    own_size = elem_size[global_elem]
    mortar_size = jnp.where(rec_sub < 4, 0.5 * own_size, own_size)
    live_rec = (rec_sub < 5).astype(jnp.float32)
    is_bound = rec_peer < 0
    is_local = rec_peer == owner_device
    is_remote = jnp.logical_and(jnp.logical_not(is_bound), jnp.logical_not(is_local))
    safe_peer = jnp.maximum(rec_peer, 0)
    link_slot = jnp.where(is_remote, (safe_peer * N_PARTS + owner_device) * capacity + rec_index, 0)
    partner_index = jnp.where(is_remote, safe_peer * rec_dev + send_rec[link_slot], safe_peer * rec_dev + rec_index)
    weight_cube = weights[:, None, None] * weights[None, :, None] * weights[None, None, :]
    face_weight = (weights[:, None] * weights[None, :]).reshape(36)
    precond_scale = inv_size[None, :] / stiff_diag[:, None]

    def apply_operator(flat_field):
        nodal_field = flat_field.reshape(6, 6, 6, elem_total)
        face_value, face_slope = face_traces(nodal_field, inv_size, derivative)
        own_traces = mortar_traces(face_value, face_slope, rec_col, rec_sub, halves)
        volume = volume_term(nodal_field, elem_size, weight_cube, derivative)
        partner = own_traces[:, partner_index]
        term_value, term_slope = mortar_terms(own_traces, partner, is_bound, mortar_size, live_rec, face_weight)
        res_value, res_slope = scatter_faces(term_value, term_slope, rec_col, rec_sub, halves, 6 * elem_total)
        lifted = lift_faces(res_value, res_slope, inv_size, derivative, elem_total)
        return (volume + lifted).reshape(216, elem_total)
    scale_total = 216.0 * elem_total

    def residual_of(solution):
        return jnp.where(live_elem[None, :], rhs - apply_operator(solution), 0.0)

    def log_norms(residual, precond):
        total_sums = jnp.stack([jnp.sum(residual * residual), jnp.sum(residual * precond)])
        return 0.5 * jnp.log(total_sums / scale_total)
    top_value = spectrum_top[0]
    bottom = top_value / BOTTOM_RATIO
    center = 0.5 * (top_value + bottom)
    radius = 0.5 * (top_value - bottom)
    sigma_ratio = center / radius
    rho_prev = 1.0 / sigma_ratio
    solution = start
    residual = residual_of(solution)
    precond = precond_scale * residual
    direction = precond / center
    rows_list = [log_norms(residual, precond)]
    for step_index in range(1, ITERS):
        solution = solution + direction
        residual = residual_of(solution)
        precond = precond_scale * residual
        rows_list.append(log_norms(residual, precond))
        rho_next = 1.0 / (2.0 * sigma_ratio - rho_prev)
        direction = rho_next * rho_prev * direction + 2.0 * rho_next / radius * precond
        rho_prev = rho_next
    solution = solution + direction
    return (solution, jnp.stack(rows_list))
```

```python
import functools
import math

import jax
import jax.numpy as jnp
import numpy as np
from jax import lax
from jax.experimental import pallas as pl
from jax.experimental.pallas import tpu as pltpu
from jax.sharding import PartitionSpec as P

ITERS = 3
REACH = 7
AXIS = "parts"
PENALTY = 36.0
BOTTOM_RATIO = 8.0
SLOPE_AT = 40
AGAIN_AT = 80
UNROLL = 32


BF = jnp.bfloat16
F32 = jnp.float32
STEPS = list(range(-REACH, 0)) + list(range(1, REACH + 1))


def lobatto_tables():
    root_seven = math.sqrt(7.0)
    inner_root = math.sqrt(1.0 / 3.0 - 2.0 * root_seven / 21.0)
    outer_root = math.sqrt(1.0 / 3.0 + 2.0 * root_seven / 21.0)
    points = (np.array([-1.0, -outer_root, -inner_root, inner_root, outer_root, 1.0]) + 1.0) / 2.0
    weights = (
        np.array(
            [
                1.0 / 15.0,
                (14.0 - root_seven) / 30.0,
                (14.0 + root_seven) / 30.0,
                (14.0 + root_seven) / 30.0,
                (14.0 - root_seven) / 30.0,
                1.0 / 15.0,
            ]
        )
        / 2.0
    )
    barycentric = np.array(
        [1.0 / np.prod([points[j] - points[k] for k in range(6) if k != j]) for j in range(6)]
    )
    derivative = np.zeros((6, 6))
    for i in range(6):
        for j in range(6):
            if i != j:
                derivative[i, j] = barycentric[j] / barycentric[i] / (points[i] - points[j])
        derivative[i, i] = -np.sum(derivative[i])
    halves = np.zeros((2, 6, 6))
    for which_half in range(2):
        targets = (points + which_half) / 2.0
        for i in range(6):
            for j in range(6):
                halves[which_half, i, j] = np.prod(
                    [(targets[i] - points[k]) / (points[j] - points[k]) for k in range(6) if k != j]
                )
    column_sums = np.sum(derivative * derivative * weights[:, None], axis=0)
    stiff_diag = (
        column_sums[:, None, None] * weights[None, :, None] * weights[None, None, :]
        + weights[:, None, None] * column_sums[None, :, None] * weights[None, None, :]
        + weights[:, None, None] * weights[None, :, None] * column_sums[None, None, :]
    )
    return (weights, derivative, halves, stiff_diag.reshape(216))


def split_const(matrix):
    high = np.asarray(matrix, np.float32).astype(BF)
    low = (np.asarray(matrix, np.float64) - high.astype(np.float64)).astype(BF)
    return high, low


def build_constants():
    weights, derivative, halves, stiff_diag = lobatto_tables()
    eye = np.eye(6)
    faces = np.zeros((256, 6 * 128))
    lift = np.zeros((6, 128, 256))
    for direction in range(6):
        axis_index = direction // 2
        layer = 5 * (direction % 2)
        value_vec = eye[layer]
        slope_vec = (2.0 * (direction % 2) - 1.0) * derivative[layer]
        for vec, places, lift_at in (
            (value_vec, (0, AGAIN_AT), 0),
            (slope_vec, (SLOPE_AT,), SLOPE_AT),
        ):
            if axis_index == 0:
                block = np.einsum("i,jp,kq->ijkpq", vec, eye, eye)
            elif axis_index == 1:
                block = np.einsum("j,ip,kq->ijkpq", vec, eye, eye)
            else:
                block = np.einsum("k,ip,jq->ijkpq", vec, eye, eye)
            block = block.reshape(216, 36)
            for place in places:
                faces[:216, direction * 128 + place : direction * 128 + place + 36] = block
            lift[direction, lift_at : lift_at + 36, :216] = block.T
    stiff = derivative.T @ np.diag(weights) @ derivative
    mass = np.diag(weights)
    volume = np.zeros((256, 256))
    volume[:216, :216] = (
        np.kron(stiff, np.kron(mass, mass))
        + np.kron(mass, np.kron(stiff, mass))
        + np.kron(mass, np.kron(mass, stiff))
    )
    onto = np.zeros((128, 4 * 128))
    off = np.zeros((5, 128, 128))
    face_weight = np.kron(weights, weights)
    for sub in range(5):
        if sub < 4:
            mortar = np.kron(halves[sub % 2], halves[sub // 2]).T
            onto[0:36, sub * 128 : sub * 128 + 36] = mortar
            onto[0:36, sub * 128 + AGAIN_AT : sub * 128 + AGAIN_AT + 36] = mortar
            onto[SLOPE_AT : SLOPE_AT + 36, sub * 128 + SLOPE_AT : sub * 128 + SLOPE_AT + 36] = mortar
        else:
            mortar = np.eye(36)
        back = face_weight[:, None] * mortar.T
        off[sub, 0:36, 0:36] = PENALTY * back
        off[sub, SLOPE_AT : SLOPE_AT + 36, 0:36] = back
        off[sub, AGAIN_AT : AGAIN_AT + 36, SLOPE_AT : SLOPE_AT + 36] = back
    faces_hi, faces_lo = split_const(faces)
    vol_hi, vol_lo = split_const(volume)
    onto_hi, onto_lo = split_const(onto)
    off_hi, off_lo = split_const(off)
    lift_hi, lift_lo = split_const(lift)
    onto_main = np.concatenate([onto_hi, onto_hi], axis=0)
    off_main = np.concatenate(
        [
            np.concatenate([off_hi, off_lo], axis=2),
            np.concatenate([off_hi, np.zeros_like(off_lo)], axis=2),
        ],
        axis=1,
    )
    lift_main = np.concatenate([lift_hi, lift_hi], axis=1)
    spread = np.zeros((30, 64, 128), np.float32)
    for slab in range(30):
        spread[slab, slab, :SLOPE_AT] = 1.0
        spread[slab, 32 + slab, SLOPE_AT:] = 1.0
    inv_diag = np.zeros((1, 256), np.float32)
    inv_diag[0, :216] = 1.0 / stiff_diag
    return dict(
        faces_hi=faces_hi,
        faces_lo=faces_lo,
        vol_hi=vol_hi,
        vol_lo=vol_lo,
        onto_main=onto_main,
        onto_lo=onto_lo,
        off_main=off_main,
        lift_main=lift_main,
        lift_lo=lift_lo,
        spread=spread.astype(BF),
        inv_diag=inv_diag,
    )


def dot(left, right):
    return lax.dot_general(left, right, (((1,), (0,)), ((), ())), preferred_element_type=F32)


def split(value):
    high = value.astype(BF)
    return high, (value - high.astype(F32)).astype(BF)


def lane_groups(elems):
    lane = lax.broadcasted_iota(jnp.int32, (elems, 128), 1)
    return lane < SLOPE_AT, lane < AGAIN_AT


def safe_inverse(size):
    return jnp.where(size > 0.0, 1.0 / jnp.maximum(size, 0.5), 0.0)


def write_tables(x, size, consts, pool, elems):
    slab = 6 * elems
    is_value, below_again = lane_groups(elems)
    is_slope = jnp.logical_and(below_again, jnp.logical_not(is_value))
    scale = jnp.where(is_slope, safe_inverse(size), 1.0)
    x_hi, x_lo = split(x)
    for pair in range(3):
        cols = slice(pair * 256, (pair + 1) * 256)
        hi = consts["faces_hi"][:, cols]
        both = dot(x_hi, hi) + dot(x_lo, hi) + dot(x_hi, consts["faces_lo"][:, cols])
        for part in range(2):
            direction = 2 * pair + part
            row = both[:, part * 128 : (part + 1) * 128] * scale
            pool[4 * slab + direction * elems : 4 * slab + (direction + 1) * elems, :] = row

    def quarters(direction, carry):
        at = pl.multiple_of(direction * elems, elems)
        row_hi, row_lo = split(pool[pl.ds(4 * slab + at, elems), :])
        both_rows = jnp.concatenate([row_hi, row_lo], axis=1)
        for pair in range(2):
            cols = slice(pair * 256, (pair + 1) * 256)
            both = dot(both_rows, consts["onto_main"][:, cols]) + dot(
                row_hi, consts["onto_lo"][:, cols]
            )
            pool[pl.ds(2 * pair * slab + at, elems), :] = both[:, :128]
            pool[pl.ds((2 * pair + 1) * slab + at, elems), :] = both[:, 128:]
        return carry

    lax.fori_loop(0, 6, quarters, 0)


def pack_rows(table_row, send_rec, info, pool, outs, capacity):
    for position, out in enumerate(outs):
        row = jnp.clip(info[0] + STEPS[position], 0, 2 * REACH)

        def chunk(k, carry, row=row, out=out):
            rows = []
            for u in range(UNROLL):
                rec = send_rec[row * capacity + k * UNROLL + u]
                rows.append(pool[pl.ds(table_row[rec], 1), :])
            for u in range(UNROLL):
                out[pl.ds(k * UNROLL + u, 1), :] = rows[u]
            return carry

        lax.fori_loop(0, capacity // UNROLL, chunk, 0)


def first_kernel(elems, capacity, records, names):
    def body(*refs):
        (start, size_ref, recs, table_row, send_rec, info) = refs[:6]
        consts = dict(zip(names, refs[6 : 6 + len(names)]))
        rest = refs[6 + len(names) :]
        x_out, counts_out, flag_out = rest[:3]
        outs = rest[3 : 3 + 2 * REACH]
        pool = rest[3 + 2 * REACH]
        size = size_ref[...]
        x = jnp.concatenate(
            [start[...].T, jnp.zeros((elems, 40), F32)], axis=1
        )
        x_out[...] = x
        write_tables(x, size, consts, pool, elems)
        pack_rows(table_row, send_rec, info, pool, outs, capacity)
        row_iota = lax.broadcasted_iota(jnp.int32, (64, records), 0)
        slabs = recs[1:2, :]
        weight = recs[2:3, :].astype(F32)
        low = jnp.where(row_iota == slabs, 1.0, 0.0)
        high = jnp.where(row_iota - 32 == slabs, 1.0, 0.0) * weight
        kinds = (low + high).astype(BF)
        elem_iota = lax.broadcasted_iota(jnp.int32, (elems, records), 0)
        onehot = jnp.where(elem_iota == recs[0:1, :], 1.0, 0.0).astype(BF)
        counts = lax.dot_general(
            onehot, kinds, (((1,), (1,)), ((), ())), preferred_element_type=F32
        )
        counts_out[...] = counts
        inner = 2.0 * counts[:, :32] - counts[:, 32:]
        flag_out[0] = jnp.where(jnp.max(inner) > 1.5, 1, 0)

    return body


def step_kernel(elems, capacity, records, names, step, last):
    slab = 6 * elems
    table_rows = 5 * slab

    def body(*refs):
        (
            x_ref,
            dirn_ref,
            rhs_ref,
            size_ref,
            counts_ref,
            flag,
            scalars,
            pool_col,
            row_list,
            dest,
            send_rec,
            info,
        ) = refs[:12]
        received = refs[12 : 12 + 2 * REACH]
        at = 12 + 2 * REACH
        consts = dict(zip(names, refs[at : at + len(names)]))
        rest = refs[at + len(names) :]
        if last:
            x_out, norm_out = rest[:2]
            outs = ()
            pool, sums, total = rest[2:]
        else:
            x_out, dirn_out, norm_out = rest[:3]
            outs = rest[3 : 3 + 2 * REACH]
            pool, sums, total = rest[3 + 2 * REACH :]
        size = size_ref[...]
        inverse = safe_inverse(size)
        x = x_ref[...]
        write_tables(x, size, consts, pool, elems)
        for position, block in enumerate(received):
            base = table_rows + position * capacity
            pool[base : base + capacity, :] = block[...]

        def clear(k, carry):
            at = pl.multiple_of(k * elems, elems)
            sums[pl.ds(at, elems), :] = jnp.zeros((elems, 128), F32)
            return carry

        lax.fori_loop(0, 30, clear, 0)

        @pl.when(flag[0] == 0)
        def _():
            def chunk(k, carry):
                base = k * UNROLL
                rows = []
                for u in range(UNROLL):
                    rows.append(pool[pl.ds(row_list[pool_col[base + u]], 1), :])
                for u in range(UNROLL):
                    sums[pl.ds(dest[base + u], 1), :] = rows[u]
                return carry

            lax.fori_loop(0, records // UNROLL, chunk, 0)

        @pl.when(flag[0] != 0)
        def _():
            def one(r, carry):
                here = pl.ds(dest[r], 1)
                sums[here, :] = sums[here, :] + pool[pl.ds(row_list[pool_col[r]], 1), :]
                return carry

            lax.fori_loop(0, records, one, 0)

        x_hi, x_lo = split(x)
        vol_hi = consts["vol_hi"][...]
        volume = dot(x_hi, vol_hi) + dot(x_lo, vol_hi) + dot(x_hi, consts["vol_lo"][...])
        size_wide = jnp.concatenate([size, size], axis=1)
        total[...] = volume * size_wide
        counts = counts_ref[...].astype(BF)
        is_value, below_again = lane_groups(elems)

        def direction_terms(direction, carry):
            at = pl.multiple_of(direction * elems, elems)
            acc = jnp.zeros((elems, 256), F32)
            for sub in range(5):
                edge = size if sub == 4 else 0.5 * size
                area = -0.5 * edge * edge
                coef = jnp.where(is_value, edge, jnp.where(below_again, area, area * inverse))
                rows = pl.ds(sub * slab + at, elems)
                times = dot(counts, consts["spread"][sub * 6 + direction])
                term = coef * (pool[rows, :] * times - sums[rows, :])
                term_hi, term_lo = split(term)
                acc = acc + dot(
                    jnp.concatenate([term_hi, term_lo], axis=1), consts["off_main"][sub]
                )
            face = acc[:, :128] + acc[:, 128:]
            face_hi, face_lo = split(face)
            total[...] += dot(
                jnp.concatenate([face_hi, face_lo], axis=1), consts["lift_main"][direction]
            ) + dot(face_hi, consts["lift_lo"][direction])
            return carry

        lax.fori_loop(0, 6, direction_terms, 0)
        rhs = jnp.concatenate([rhs_ref[...].T, jnp.zeros((elems, 40), F32)], axis=1)
        residual = jnp.where(size_wide > 0.0, rhs - total[...], 0.0)
        scaled = residual * (jnp.concatenate([inverse, inverse], axis=1) * consts["inv_diag"][...])

        def fold(product):
            part = jnp.sum(product.reshape(elems // 8, 8, 256), axis=0)
            return part[:, :128] + part[:, 128:]

        norm_out[0:8, :] = fold(residual * residual)
        norm_out[8:16, :] = fold(residual * scaled)
        dirn = scalars[2 * step + 1] * scaled
        if step > 0:
            dirn = scalars[2 * step] * dirn_ref[...] + dirn
        x_new = x + dirn
        if last:
            x_out[...] = x_new[:, :216].T
        else:
            x_out[...] = x_new
            dirn_out[...] = dirn
            write_tables(x_new, size, consts, pool, elems)
            pack_rows(row_list, send_rec, info, pool, outs, capacity)

    return body


def on_device(
    rhs, start, spectrum_top, elem_code, rec_elem, rec_dir, rec_sub, rec_peer, rec_index, send_rec
):
    consts = build_constants()
    names = tuple(consts)
    first_names = ("faces_hi", "faces_lo", "onto_main", "onto_lo")
    parts = lax.axis_size(AXIS)
    own = lax.axis_index(AXIS)
    elems = rhs.shape[1]
    records = rec_elem.shape[0]
    capacity = send_rec.shape[0] // parts
    slab = 6 * elems
    table_rows = 5 * slab
    slots = 2 * REACH * capacity

    size = jnp.broadcast_to((0.5 * elem_code.astype(F32))[:, None], (elems, 128))
    sub = jnp.minimum(rec_sub, 4)
    table_row = sub * slab + rec_dir * elems + rec_elem
    live = rec_sub < 5
    bound = rec_peer < 0
    offset = own - rec_peer
    position = jnp.where(offset < 0, offset + REACH, offset + REACH - 1)
    remote_col = records + jnp.clip(position, 0, 2 * REACH - 1) * capacity + rec_index
    pool_col = jnp.where(rec_peer == own, rec_index, jnp.where(bound, 0, remote_col))
    dest = jnp.where(jnp.logical_and(live, jnp.logical_not(bound)), table_row, table_rows)
    row_list = jnp.concatenate([table_row, table_rows + jnp.arange(slots, dtype=jnp.int32)])
    kind = jnp.where(live, sub * 6 + rec_dir, 99)
    recs = jnp.stack([rec_elem, kind, jnp.where(bound, 2, 1)])
    first_row = jnp.clip(own - REACH, 0, parts - 1 - 2 * REACH)
    lists = lax.dynamic_slice(
        send_rec.reshape(parts, capacity), (first_row, 0), (2 * REACH + 1, capacity)
    ).reshape(-1)
    info = (own - first_row).astype(jnp.int32).reshape(1)

    top_value = spectrum_top[0]
    bottom = top_value / BOTTOM_RATIO
    center = 0.5 * (top_value + bottom)
    radius = 0.5 * (top_value - bottom)
    sigma_ratio = center / radius
    rho_prev = 1.0 / sigma_ratio
    factors = [jnp.zeros((), F32), 1.0 / center]
    for _ in range(1, ITERS):
        rho_next = 1.0 / (2.0 * sigma_ratio - rho_prev)
        factors += [rho_next * rho_prev, 2.0 * rho_next / radius]
        rho_prev = rho_next
    factors = jnp.stack(factors)

    vmem = pl.BlockSpec(memory_space=pltpu.VMEM)
    smem = pl.BlockSpec(memory_space=pltpu.SMEM)
    field = jax.ShapeDtypeStruct((elems, 256), F32)
    block = jax.ShapeDtypeStruct((capacity, 128), F32)
    params = pltpu.CompilerParams(vmem_limit_bytes=58 << 20)
    pool_shape = pltpu.VMEM((table_rows + slots, 128), F32)
    sums_shape = pltpu.VMEM((table_rows + 8, 128), F32)

    x, counts, flag, *blocks = pl.pallas_call(
        first_kernel(elems, capacity, records, first_names),
        name="first_traces",
        out_shape=(
            field,
            jax.ShapeDtypeStruct((elems, 64), F32),
            jax.ShapeDtypeStruct((1,), jnp.int32),
        )
        + (block,) * (2 * REACH),
        in_specs=[vmem] * 3 + [smem] * 3 + [vmem] * len(first_names),
        out_specs=(vmem, vmem, smem) + (vmem,) * (2 * REACH),
        scratch_shapes=[pool_shape],
        compiler_params=params,
    )(start, size, recs, table_row, lists, info, *[consts[n] for n in first_names])

    dirn = x
    norms = []
    for step in range(ITERS):
        last = step == ITERS - 1
        received = [
            lax.ppermute(piece, AXIS, [(i, (i + by) % parts) for i in range(parts)])
            for piece, by in zip(blocks, STEPS)
        ]
        norm_shape = jax.ShapeDtypeStruct((16, 128), F32)
        if last:
            shapes = (jax.ShapeDtypeStruct((216, elems), F32), norm_shape)
        else:
            shapes = (field, field, norm_shape) + (block,) * (2 * REACH)
        results = pl.pallas_call(
            step_kernel(elems, capacity, records, names, step, last),
            name="smoother_step_%d" % step,
            out_shape=shapes,
            in_specs=[vmem] * 5
            + [smem] * 7
            + [vmem] * (2 * REACH)
            + [vmem] * len(names),
            out_specs=(vmem,) * len(shapes),
            scratch_shapes=[pool_shape, sums_shape, pltpu.VMEM((elems, 256), F32)],
            compiler_params=params,
        )(
            x,
            dirn,
            rhs,
            size,
            counts,
            flag,
            factors,
            pool_col,
            row_list,
            dest,
            lists,
            info,
            *received,
            *[consts[n] for n in names],
        )
        if last:
            answer, norm = results
        else:
            x, dirn, norm, *blocks = results
        norms.append(norm)

    sums = jnp.stack([jnp.sum(n.reshape(2, 8 * 128), axis=1) for n in norms]).reshape(1, 6)
    mine = jnp.broadcast_to(jnp.pad(sums, ((0, 0), (0, 122))), (parts, 128))
    gathered = lax.all_to_all(mine, AXIS, 0, 0, tiled=True)
    total = jnp.sum(gathered, axis=0)[:6].reshape(3, 2)
    return (answer, 0.5 * jnp.log(total / (216.0 * elems * parts)))


def solution(mesh):
    split_spec = P(AXIS)
    in_specs = (P(None, AXIS), P(None, AXIS), P()) + (split_spec,) * 7
    out_specs = (P(None, AXIS), P())
    return jax.shard_map(
        on_device, mesh=mesh, in_specs=in_specs, out_specs=out_specs, check_vma=False
    )
```

```python
import functools
import math

import jax
import jax.numpy as jnp
import numpy as np
from jax import lax
from jax.experimental import pallas as pl
from jax.experimental.pallas import tpu as pltpu
from jax.sharding import PartitionSpec as P

ITERS = 3
REACH = 7
AXIS = "parts"
PENALTY = 36.0
BOTTOM_RATIO = 8.0
SLOPE_AT = 40
AGAIN_AT = 80
UNROLL = 32


BF = jnp.bfloat16
F32 = jnp.float32
STEPS = list(range(1, REACH + 1)) + list(range(-REACH, 0))
VMEM_MIB = 16
SMALL_MIB = 16
PAIR_BITS = 14


def lobatto_tables():
    root_seven = math.sqrt(7.0)
    inner_root = math.sqrt(1.0 / 3.0 - 2.0 * root_seven / 21.0)
    outer_root = math.sqrt(1.0 / 3.0 + 2.0 * root_seven / 21.0)
    points = (np.array([-1.0, -outer_root, -inner_root, inner_root, outer_root, 1.0]) + 1.0) / 2.0
    weights = (
        np.array(
            [
                1.0 / 15.0,
                (14.0 - root_seven) / 30.0,
                (14.0 + root_seven) / 30.0,
                (14.0 + root_seven) / 30.0,
                (14.0 - root_seven) / 30.0,
                1.0 / 15.0,
            ]
        )
        / 2.0
    )
    barycentric = np.array(
        [1.0 / np.prod([points[j] - points[k] for k in range(6) if k != j]) for j in range(6)]
    )
    derivative = np.zeros((6, 6))
    for i in range(6):
        for j in range(6):
            if i != j:
                derivative[i, j] = barycentric[j] / barycentric[i] / (points[i] - points[j])
        derivative[i, i] = -np.sum(derivative[i])
    halves = np.zeros((2, 6, 6))
    for which_half in range(2):
        targets = (points + which_half) / 2.0
        for i in range(6):
            for j in range(6):
                halves[which_half, i, j] = np.prod(
                    [(targets[i] - points[k]) / (points[j] - points[k]) for k in range(6) if k != j]
                )
    column_sums = np.sum(derivative * derivative * weights[:, None], axis=0)
    stiff_diag = (
        column_sums[:, None, None] * weights[None, :, None] * weights[None, None, :]
        + weights[:, None, None] * column_sums[None, :, None] * weights[None, None, :]
        + weights[:, None, None] * weights[None, :, None] * column_sums[None, None, :]
    )
    return (weights, derivative, halves, stiff_diag.reshape(216))


def split_const(matrix):
    high = np.asarray(matrix, np.float32).astype(BF)
    low = (np.asarray(matrix, np.float64) - high.astype(np.float64)).astype(BF)
    return high, low


def build_constants():
    weights, derivative, halves, stiff_diag = lobatto_tables()
    eye = np.eye(6)
    faces = np.zeros((256, 6 * 128))
    lift = np.zeros((6, 128, 256))
    for direction in range(6):
        axis_index = direction // 2
        layer = 5 * (direction % 2)
        value_vec = eye[layer]
        slope_vec = (2.0 * (direction % 2) - 1.0) * derivative[layer]
        for vec, places, lift_at in (
            (value_vec, (0, AGAIN_AT), 0),
            (slope_vec, (SLOPE_AT,), SLOPE_AT),
        ):
            if axis_index == 0:
                block = np.einsum("i,jp,kq->ijkpq", vec, eye, eye)
            elif axis_index == 1:
                block = np.einsum("j,ip,kq->ijkpq", vec, eye, eye)
            else:
                block = np.einsum("k,ip,jq->ijkpq", vec, eye, eye)
            block = block.reshape(216, 36)
            for place in places:
                faces[:216, direction * 128 + place : direction * 128 + place + 36] = block
            lift[direction, lift_at : lift_at + 36, :216] = block.T
    stiff = derivative.T @ np.diag(weights) @ derivative
    mass = np.diag(weights)
    volume = np.zeros((256, 256))
    volume[:216, :216] = (
        np.kron(stiff, np.kron(mass, mass))
        + np.kron(mass, np.kron(stiff, mass))
        + np.kron(mass, np.kron(mass, stiff))
    )
    onto = np.zeros((128, 4 * 128))
    off = np.zeros((5, 128, 128))
    face_weight = np.kron(weights, weights)
    for sub in range(5):
        if sub < 4:
            mortar = np.kron(halves[sub % 2], halves[sub // 2]).T
            onto[0:36, sub * 128 : sub * 128 + 36] = mortar
            onto[0:36, sub * 128 + AGAIN_AT : sub * 128 + AGAIN_AT + 36] = mortar
            onto[SLOPE_AT : SLOPE_AT + 36, sub * 128 + SLOPE_AT : sub * 128 + SLOPE_AT + 36] = mortar
        else:
            mortar = np.eye(36)
        back = face_weight[:, None] * mortar.T
        off[sub, 0:36, 0:36] = PENALTY * back
        off[sub, SLOPE_AT : SLOPE_AT + 36, 0:36] = back
        off[sub, AGAIN_AT : AGAIN_AT + 36, SLOPE_AT : SLOPE_AT + 36] = back
    faces_hi, faces_lo = split_const(faces)
    vol_hi, vol_lo = split_const(volume)
    onto_hi, onto_lo = split_const(onto)
    off_hi, off_lo = split_const(off)
    lift_hi, lift_lo = split_const(lift)
    onto_main = np.concatenate([onto_hi, onto_hi], axis=0)
    off_main = np.concatenate(
        [
            np.concatenate([off_hi, off_lo], axis=2),
            np.concatenate([off_hi, np.zeros_like(off_lo)], axis=2),
        ],
        axis=1,
    )
    lift_main = np.concatenate([lift_hi, lift_hi], axis=1)
    spread = np.zeros((30, 64, 128), np.float32)
    for slab in range(30):
        spread[slab, slab, :SLOPE_AT] = 1.0
        spread[slab, 32 + slab, SLOPE_AT:] = 1.0
    inv_diag = np.zeros((1, 256), np.float32)
    inv_diag[0, :216] = 1.0 / stiff_diag
    return dict(
        faces_hi=faces_hi,
        faces_lo=faces_lo,
        vol_hi=vol_hi,
        vol_lo=vol_lo,
        onto_main=onto_main,
        onto_lo=onto_lo,
        off_main=off_main,
        lift_main=lift_main,
        lift_lo=lift_lo,
        spread=spread.astype(BF),
        inv_diag=inv_diag,
    )


def dot(left, right):
    return lax.dot_general(left, right, (((1,), (0,)), ((), ())), preferred_element_type=F32)


def split(value):
    high = value.astype(BF)
    return high, (value - high.astype(F32)).astype(BF)


def lane_groups(elems):
    lane = lax.broadcasted_iota(jnp.int32, (elems, 128), 1)
    return lane < SLOPE_AT, lane < AGAIN_AT


def safe_inverse(size):
    return jnp.where(size > 0.0, 1.0 / jnp.maximum(size, 0.5), 0.0)


def write_tables(x, size, consts, pool, elems):
    slab = 6 * elems
    is_value, below_again = lane_groups(elems)
    is_slope = jnp.logical_and(below_again, jnp.logical_not(is_value))
    scale = jnp.where(is_slope, safe_inverse(size), 1.0)
    x_hi, x_lo = split(x)
    for pair in range(3):
        cols = slice(pair * 256, (pair + 1) * 256)
        hi = consts["faces_hi"][:, cols]
        both = dot(x_hi, hi) + dot(x_lo, hi) + dot(x_hi, consts["faces_lo"][:, cols])
        for part in range(2):
            direction = 2 * pair + part
            row = both[:, part * 128 : (part + 1) * 128] * scale
            pool[4 * slab + direction * elems : 4 * slab + (direction + 1) * elems, :] = row

    def quarters(direction, carry):
        at = pl.multiple_of(direction * elems, elems)
        row_hi, row_lo = split(pool[pl.ds(4 * slab + at, elems), :])
        both_rows = jnp.concatenate([row_hi, row_lo], axis=1)
        for pair in range(2):
            cols = slice(pair * 256, (pair + 1) * 256)
            both = dot(both_rows, consts["onto_main"][:, cols]) + dot(
                row_hi, consts["onto_lo"][:, cols]
            )
            pool[pl.ds(2 * pair * slab + at, elems), :] = both[:, :128]
            pool[pl.ds((2 * pair + 1) * slab + at, elems), :] = both[:, 128:]
        return carry

    lax.fori_loop(0, 6, quarters, 0)


class Fetch:
    def __init__(self, names, sources, targets, sems):
        self.copies = {
            name: pltpu.make_async_copy(source, target, sems.at[i])
            for i, (name, source, target) in enumerate(zip(names, sources, targets))
        }

    def start(self):
        for copy in self.copies.values():
            copy.start()

    def wait(self, *names):
        for name in names:
            self.copies.pop(name).wait()


def pack_rows(table_row, send_rec, info, pool, staging, outs, sems, capacity):
    copies = []
    for position, out in enumerate(outs):
        row = jnp.clip(info[0] + STEPS[position], 0, 2 * REACH)

        def chunk(k, carry, row=row, position=position):
            rows = []
            for u in range(UNROLL):
                rec = send_rec[row * capacity + k * UNROLL + u]
                rows.append(pool[pl.ds(table_row[rec], 1), :])
            for u in range(UNROLL):
                staging[pl.ds(position * capacity + k * UNROLL + u, 1), :] = rows[u]
            return carry

        lax.fori_loop(0, capacity // UNROLL, chunk, 0)
        here = staging.at[position * capacity : (position + 1) * capacity, :]
        copies.append(pltpu.make_async_copy(here, out, sems.at[position]))
        copies[-1].start()
    for copy in copies:
        copy.wait()


FIRST_NAMES = ("faces_hi", "faces_lo", "onto_main", "onto_lo")
LAST_NAMES = ("off_main", "spread", "lift_main", "lift_lo")


def first_kernel(elems, capacity):
    def body(*refs):
        start, size_ref, table_row, send_rec, info = refs[:5]
        consts = dict(zip(FIRST_NAMES, refs[5 : 5 + len(FIRST_NAMES)]))
        x_out, pool, *rest = refs[5 + len(FIRST_NAMES) :]
        outs = rest[: 2 * REACH]
        staging, out_sems = rest[2 * REACH :]
        x = jnp.concatenate([start[...].T, jnp.zeros((elems, 40), F32)], axis=1)
        x_out[...] = x
        write_tables(x, size_ref[...], consts, pool, elems)
        pack_rows(table_row, send_rec, info, pool, staging, outs, out_sems, capacity)

    return body


def add_rows(flag, count, source, target, pool, sums):
    @pl.when(flag == 0)
    def _():
        def chunk(k, carry):
            base = k * UNROLL
            rows = []
            for u in range(UNROLL):
                rows.append(pool[pl.ds(source(base + u), 1), :])
            for u in range(UNROLL):
                sums[pl.ds(target(base + u), 1), :] = rows[u]
            return carry

        lax.fori_loop(0, (count + UNROLL - 1) // UNROLL, chunk, 0)

    @pl.when(flag != 0)
    def _():
        def one(r, carry):
            here = pl.ds(target(r), 1)
            sums[here, :] = sums[here, :] + pool[pl.ds(source(r), 1), :]
            return carry

        lax.fori_loop(0, count, one, 0)


def inner_kernel(elems, records, compact):
    table_rows = 30 * elems

    def body(*refs):
        if compact:
            x_ref, size_ref, pool, table_row, local_rec, local_row, far_pair, recs = refs[:8]
            vol_hi, vol_lo = refs[8:10]
            sums, total, far_pairs, far_count, counts_out, flag_out = refs[10:]
        else:
            x_ref, size_ref, pool, table_row, local_rec, local_row, flag_ref = refs[:7]
            vol_hi, vol_lo = refs[7:9]
            sums, total = refs[9:]
        if compact:
            row_iota = lax.broadcasted_iota(jnp.int32, (64, records), 0)
            slabs = recs[1:2, :]
            weight = recs[2:3, :].astype(F32)
            low = jnp.where(row_iota == slabs, 1.0, 0.0)
            high = jnp.where(row_iota - 32 == slabs, 1.0, 0.0) * weight
            kinds = (low + high).astype(BF)
            elem_iota = lax.broadcasted_iota(jnp.int32, (elems, records), 0)
            onehot = jnp.where(elem_iota == recs[0:1, :], 1.0, 0.0).astype(BF)
            counts = lax.dot_general(
                onehot, kinds, (((1,), (1,)), ((), ())), preferred_element_type=F32
            )
            counts_out[...] = counts
            paired = 2.0 * counts[:, :32] - counts[:, 32:]
            flag = jnp.where(jnp.max(paired) > 1.5, 1, 0)
            flag_out[0] = flag
        else:
            flag = flag_ref[0]

        def clear(k, carry):
            at = pl.multiple_of(k * elems, elems)
            sums[pl.ds(at, elems), :] = jnp.zeros((elems, 128), F32)
            return carry

        lax.fori_loop(0, 30, clear, 0)
        sums[table_rows : table_rows + 8, :] = jnp.zeros((8, 128), F32)
        add_rows(
            flag,
            records,
            lambda r: table_row[local_rec[r]],
            lambda r: local_row[r],
            pool,
            sums,
        )
        x_hi, x_lo = split(x_ref[...])
        hi = vol_hi[...]
        volume = dot(x_hi, hi) + dot(x_lo, hi) + dot(x_hi, vol_lo[...])
        size = size_ref[...]
        total[...] = volume * jnp.concatenate([size, size], axis=1)
        if compact:

            def collect(k, count):
                pairs = [far_pair[k * 16 + u] for u in range(16)]
                for pair in pairs:
                    far_pairs[count] = pair
                    count = count + jnp.where(pair >= 0, 1, 0)
                return count

            count = lax.fori_loop(0, records // 16, collect, 0)
            for u in range(UNROLL):
                far_pairs[count + u] = table_rows
            far_count[0] = count

    return body


def outer_kernel(elems, capacity, step, last):
    slab = 6 * elems
    table_rows = 5 * slab
    const_names = LAST_NAMES if last else LAST_NAMES + FIRST_NAMES
    block_names = tuple("block%d" % i for i in range(2 * REACH))

    def body(*refs):
        x_ref, dirn_ref, rhs_ref, size_ref, counts_ref, pool, near, volume, inv_diag = refs[:9]
        flag, scalars, far_pairs, far_count, table_row, send_rec, info = refs[9:16]
        received = refs[16 : 16 + 2 * REACH]
        at = 16 + 2 * REACH
        consts = dict(zip(const_names, refs[at : at + len(const_names)]))
        rest = refs[at + len(const_names) :]
        if last:
            earlier = rest[: ITERS - 1]
            sums, x_out, norm_out = rest[ITERS - 1 : ITERS + 2]
            rest = rest[ITERS + 2 :]
        else:
            sums, x_out, dirn_out, norm_out, pool_out = rest[:5]
            outs = rest[5 : 5 + 2 * REACH]
            rest = rest[5 + 2 * REACH :]
        blocks, total, sems, out_sems = rest
        fetch = Fetch(
            block_names,
            received,
            [blocks.at[i * capacity : (i + 1) * capacity, :] for i in range(2 * REACH)],
            sems,
        )
        fetch.start()
        size = size_ref[...]
        inverse = safe_inverse(size)
        fetch.wait(*block_names)
        add_rows(
            flag[0],
            far_count[0],
            lambda r: far_pairs[r] >> PAIR_BITS,
            lambda r: far_pairs[r] & ((1 << PAIR_BITS) - 1),
            blocks,
            sums,
        )
        size_wide = jnp.concatenate([size, size], axis=1)
        total[...] = volume[...]
        counts = counts_ref[...].astype(BF)
        is_value, below_again = lane_groups(elems)

        def direction_terms(direction, carry):
            at = pl.multiple_of(direction * elems, elems)
            acc = jnp.zeros((elems, 256), F32)
            for sub in range(5):
                edge = size if sub == 4 else 0.5 * size
                area = -0.5 * edge * edge
                coef = jnp.where(is_value, edge, jnp.where(below_again, area, area * inverse))
                rows = pl.ds(sub * slab + at, elems)
                times = dot(counts, consts["spread"][sub * 6 + direction])
                term = coef * (pool[rows, :] * times - sums[rows, :])
                term_hi, term_lo = split(term)
                acc = acc + dot(
                    jnp.concatenate([term_hi, term_lo], axis=1), consts["off_main"][sub]
                )
            face = acc[:, :128] + acc[:, 128:]
            face_hi, face_lo = split(face)
            total[...] += dot(
                jnp.concatenate([face_hi, face_lo], axis=1), consts["lift_main"][direction]
            ) + dot(face_hi, consts["lift_lo"][direction])
            return carry

        lax.fori_loop(0, 6, direction_terms, 0)
        rhs = jnp.concatenate([rhs_ref[...].T, jnp.zeros((elems, 40), F32)], axis=1)
        residual = jnp.where(size_wide > 0.0, rhs - total[...], 0.0)
        scaled = residual * (jnp.concatenate([inverse, inverse], axis=1) * inv_diag[...])

        def fold(product):
            part = jnp.sum(product.reshape(elems // 8, 8, 256), axis=0)
            return part[:, :128] + part[:, 128:]

        folded = (fold(residual * residual), fold(residual * scaled))
        if last:
            pieces = [n[at : at + 8, :] for n in earlier for at in (0, 8)] + list(folded)
            lane = lax.broadcasted_iota(jnp.int32, norm_out.shape, 1)
            row = jnp.zeros(norm_out.shape, F32)
            for i, piece in enumerate(pieces):
                row = jnp.where(lane == i, jnp.sum(piece), row)
            norm_out[...] = row
        else:
            norm_out[0:8, :] = folded[0]
            norm_out[8:16, :] = folded[1]
        dirn = scalars[2 * step + 1] * scaled
        if step > 0:
            dirn = scalars[2 * step] * dirn_ref[...] + dirn
        x_new = x_ref[...] + dirn
        if last:
            x_out[...] = x_new[:, :216].T
        else:
            x_out[...] = x_new
            dirn_out[...] = dirn
            write_tables(x_new, size, consts, pool_out, elems)
            pack_rows(table_row, send_rec, info, pool_out, blocks, outs, out_sems, capacity)

    return body


def on_device(
    rhs, start, spectrum_top, elem_code, rec_elem, rec_dir, rec_sub, rec_peer, rec_index, send_rec
):
    consts = build_constants()
    parts = lax.axis_size(AXIS)
    own = lax.axis_index(AXIS)
    elems = rhs.shape[1]
    records = rec_elem.shape[0]
    capacity = send_rec.shape[0] // parts
    slab = 6 * elems
    table_rows = 5 * slab

    size = jnp.broadcast_to((0.5 * elem_code.astype(F32))[:, None], (elems, 128))
    sub = jnp.minimum(rec_sub, 4)
    table_row = sub * slab + rec_dir * elems + rec_elem
    live = rec_sub < 5
    bound = rec_peer < 0
    local = jnp.logical_and(rec_peer == own, live)
    far = jnp.logical_and(jnp.logical_not(bound), rec_peer != own)
    far = jnp.logical_and(far, live)
    offset = own - rec_peer
    position = jnp.where(offset > 0, offset - 1, 2 * REACH + offset)
    far_row = jnp.clip(position, 0, 2 * REACH - 1) * capacity + rec_index
    far_pair = jnp.where(far, far_row * (1 << PAIR_BITS) + table_row, -1)
    local_rec = jnp.where(local, rec_index, 0)
    local_row = jnp.where(local, table_row, table_rows)
    kind = jnp.where(live, sub * 6 + rec_dir, 99)
    recs = jnp.stack([rec_elem, kind, jnp.where(bound, 2, 1)])
    first_row = jnp.clip(own - REACH, 0, parts - 1 - 2 * REACH)
    lists = lax.dynamic_slice(
        send_rec.reshape(parts, capacity), (first_row, 0), (2 * REACH + 1, capacity)
    ).reshape(-1)
    info = (own - first_row).astype(jnp.int32).reshape(1)

    top_value = spectrum_top[0]
    bottom = top_value / BOTTOM_RATIO
    center = 0.5 * (top_value + bottom)
    radius = 0.5 * (top_value - bottom)
    sigma_ratio = center / radius
    rho_prev = 1.0 / sigma_ratio
    factors = [jnp.zeros((), F32), 1.0 / center]
    for _ in range(1, ITERS):
        rho_next = 1.0 / (2.0 * sigma_ratio - rho_prev)
        factors += [rho_next * rho_prev, 2.0 * rho_next / radius]
        rho_prev = rho_next
    factors = jnp.stack(factors)
    (size, table_row, far_pair, local_rec, local_row, recs, lists, info, factors, start) = (
        lax.optimization_barrier(
            (size, table_row, far_pair, local_rec, local_row, recs, lists, info, factors, start)
        )
    )

    vmem = pl.BlockSpec(memory_space=pltpu.VMEM)
    smem = pl.BlockSpec(memory_space=pltpu.SMEM)
    hbm = pl.BlockSpec(memory_space=pltpu.HBM)
    field = jax.ShapeDtypeStruct((elems, 256), F32)
    block = jax.ShapeDtypeStruct((capacity, 128), F32)
    table = jax.ShapeDtypeStruct((table_rows, 128), F32)
    table_more = jax.ShapeDtypeStruct((table_rows + 8, 128), F32)
    one = jax.ShapeDtypeStruct((1,), jnp.int32)
    params = pltpu.CompilerParams(vmem_limit_bytes=VMEM_MIB << 20)
    small = pltpu.CompilerParams(vmem_limit_bytes=SMALL_MIB << 20)
    staging = pltpu.VMEM((2 * REACH * capacity, 128), F32)
    blocks_out = (block,) * (2 * REACH)
    nodes = rhs.shape[0]

    def pick(names):
        return [consts[n] for n in names]

    def sems(count):
        return pltpu.SemaphoreType.DMA((count,))

    x, pool, *blocks = pl.pallas_call(
        first_kernel(elems, capacity),
        name="first_traces",
        out_shape=(field, table) + blocks_out,
        in_specs=[vmem, vmem] + [smem] * 3 + [vmem] * len(FIRST_NAMES),
        out_specs=(vmem, vmem) + (hbm,) * (2 * REACH),
        scratch_shapes=[staging, sems(2 * REACH)],
        compiler_params=small,
    )(start, size, table_row, lists, info, *pick(FIRST_NAMES))

    dirn = x
    norms = []
    for step in range(ITERS):
        last = step == ITERS - 1
        compact = step == 0
        received = [
            lax.ppermute(piece, AXIS, [(i, (i + by) % parts) for i in range(parts)])
            for piece, by in zip(blocks, STEPS)
        ]
        ints = jax.ShapeDtypeStruct((records + UNROLL,), jnp.int32)
        results = pl.pallas_call(
            inner_kernel(elems, records, compact),
            name="inner_%d" % step,
            out_shape=(table_more, field)
            + ((ints, one, jax.ShapeDtypeStruct((elems, 64), F32), one) if compact else ()),
            in_specs=[vmem] * 3
            + ([smem] * 4 + [vmem] if compact else [smem] * 4)
            + [vmem] * 2,
            out_specs=(vmem, vmem) + ((smem, smem, vmem, smem) if compact else ()),
            compiler_params=small,
            cost_estimate=pl.CostEstimate(
                flops=10**10, transcendentals=0, bytes_accessed=10**6
            ),
        )(
            x,
            size,
            pool,
            table_row,
            local_rec,
            local_row,
            *([far_pair, recs] if compact else [flag]),
            *pick(("vol_hi", "vol_lo")),
        )
        near, volume = results[:2]
        if compact:
            *far_lists, counts, flag = results[2:]
        norm_shape = jax.ShapeDtypeStruct((16, 128), F32)
        if last:
            shapes = (
                table_more,
                jax.ShapeDtypeStruct((nodes, elems), F32),
                jax.ShapeDtypeStruct((parts, 128), F32),
            )
            out_specs = (vmem,) * 3
        else:
            shapes = (table_more, field, field, norm_shape, table) + blocks_out
            out_specs = (vmem,) * 5 + (hbm,) * (2 * REACH)
        names = LAST_NAMES if last else LAST_NAMES + FIRST_NAMES
        results = pl.pallas_call(
            outer_kernel(elems, capacity, step, last),
            name="outer_%d" % step,
            out_shape=shapes,
            in_specs=[vmem] * 9
            + [smem] * 7
            + [hbm] * (2 * REACH)
            + [vmem] * (len(names) + (len(norms) if last else 0)),
            out_specs=out_specs,
            scratch_shapes=[
                staging,
                pltpu.VMEM((elems, 256), F32),
                sems(2 * REACH),
                sems(2 * REACH),
            ],
            input_output_aliases={6: 0},
            compiler_params=params,
        )(
            x,
            dirn,
            rhs,
            size,
            counts,
            pool,
            near,
            volume,
            consts["inv_diag"],
            flag,
            factors,
            *far_lists,
            table_row,
            lists,
            info,
            *received,
            *pick(names),
            *(norms if last else ()),
        )
        if last:
            _, answer, mine = results
        else:
            _, x, dirn, norm, pool, *blocks = results
            norms.append(norm)

    gathered = lax.all_to_all(mine, AXIS, 0, 0, tiled=True)
    total = jnp.sum(gathered, axis=0)[:6].reshape(3, 2)
    return (answer, 0.5 * jnp.log(total / (216.0 * elems * parts)))


def solution(mesh):
    split_spec = P(AXIS)
    in_specs = (P(None, AXIS), P(None, AXIS), P()) + (split_spec,) * 7
    out_specs = (P(None, AXIS), P())
    return jax.shard_map(
        on_device, mesh=mesh, in_specs=in_specs, out_specs=out_specs, check_vma=False
    )
```

```python
import functools
import math

import jax
import jax.numpy as jnp
import numpy as np
from jax import lax
from jax.experimental import pallas as pl
from jax.experimental.pallas import tpu as pltpu
from jax.sharding import PartitionSpec as P

ITERS = 3
REACH = 7
AXIS = "parts"
PENALTY = 36.0
BOTTOM_RATIO = 8.0
SLOPE_AT = 40
AGAIN_AT = 80
UNROLL = 32
PACK_UNROLL = 64


BF = jnp.bfloat16
F32 = jnp.float32
STEPS = list(range(1, REACH + 1)) + list(range(-REACH, 0))
VMEM_MIB = 10
SMALL_MIB = 10
PAIR_BITS = 14


def lobatto_tables():
    root_seven = math.sqrt(7.0)
    inner_root = math.sqrt(1.0 / 3.0 - 2.0 * root_seven / 21.0)
    outer_root = math.sqrt(1.0 / 3.0 + 2.0 * root_seven / 21.0)
    points = (np.array([-1.0, -outer_root, -inner_root, inner_root, outer_root, 1.0]) + 1.0) / 2.0
    weights = (
        np.array(
            [
                1.0 / 15.0,
                (14.0 - root_seven) / 30.0,
                (14.0 + root_seven) / 30.0,
                (14.0 + root_seven) / 30.0,
                (14.0 - root_seven) / 30.0,
                1.0 / 15.0,
            ]
        )
        / 2.0
    )
    barycentric = np.array(
        [1.0 / np.prod([points[j] - points[k] for k in range(6) if k != j]) for j in range(6)]
    )
    derivative = np.zeros((6, 6))
    for i in range(6):
        for j in range(6):
            if i != j:
                derivative[i, j] = barycentric[j] / barycentric[i] / (points[i] - points[j])
        derivative[i, i] = -np.sum(derivative[i])
    halves = np.zeros((2, 6, 6))
    for which_half in range(2):
        targets = (points + which_half) / 2.0
        for i in range(6):
            for j in range(6):
                halves[which_half, i, j] = np.prod(
                    [(targets[i] - points[k]) / (points[j] - points[k]) for k in range(6) if k != j]
                )
    column_sums = np.sum(derivative * derivative * weights[:, None], axis=0)
    stiff_diag = (
        column_sums[:, None, None] * weights[None, :, None] * weights[None, None, :]
        + weights[:, None, None] * column_sums[None, :, None] * weights[None, None, :]
        + weights[:, None, None] * weights[None, :, None] * column_sums[None, None, :]
    )
    return (weights, derivative, halves, stiff_diag.reshape(216))


def split_const(matrix):
    high = np.asarray(matrix, np.float32).astype(BF)
    low = (np.asarray(matrix, np.float64) - high.astype(np.float64)).astype(BF)
    return high, low


def build_constants():
    weights, derivative, halves, stiff_diag = lobatto_tables()
    eye = np.eye(6)
    faces = np.zeros((256, 6 * 128))
    lift = np.zeros((6, 128, 256))
    for direction in range(6):
        axis_index = direction // 2
        layer = 5 * (direction % 2)
        value_vec = eye[layer]
        slope_vec = (2.0 * (direction % 2) - 1.0) * derivative[layer]
        for vec, places, lift_at in (
            (value_vec, (0, AGAIN_AT), 0),
            (slope_vec, (SLOPE_AT,), SLOPE_AT),
        ):
            if axis_index == 0:
                block = np.einsum("i,jp,kq->ijkpq", vec, eye, eye)
            elif axis_index == 1:
                block = np.einsum("j,ip,kq->ijkpq", vec, eye, eye)
            else:
                block = np.einsum("k,ip,jq->ijkpq", vec, eye, eye)
            block = block.reshape(216, 36)
            for place in places:
                faces[:216, direction * 128 + place : direction * 128 + place + 36] = block
            lift[direction, lift_at : lift_at + 36, :216] = block.T
    stiff = derivative.T @ np.diag(weights) @ derivative
    mass = np.diag(weights)
    volume = np.zeros((256, 256))
    volume[:216, :216] = (
        np.kron(stiff, np.kron(mass, mass))
        + np.kron(mass, np.kron(stiff, mass))
        + np.kron(mass, np.kron(mass, stiff))
    )
    onto = np.zeros((128, 4 * 128))
    off = np.zeros((5, 128, 128))
    face_weight = np.kron(weights, weights)
    for sub in range(5):
        if sub < 4:
            mortar = np.kron(halves[sub % 2], halves[sub // 2]).T
            onto[0:36, sub * 128 : sub * 128 + 36] = mortar
            onto[0:36, sub * 128 + AGAIN_AT : sub * 128 + AGAIN_AT + 36] = mortar
            onto[SLOPE_AT : SLOPE_AT + 36, sub * 128 + SLOPE_AT : sub * 128 + SLOPE_AT + 36] = mortar
        else:
            mortar = np.eye(36)
        back = face_weight[:, None] * mortar.T
        off[sub, 0:36, 0:36] = PENALTY * back
        off[sub, SLOPE_AT : SLOPE_AT + 36, 0:36] = back
        off[sub, AGAIN_AT : AGAIN_AT + 36, SLOPE_AT : SLOPE_AT + 36] = back
    faces_hi, faces_lo = split_const(faces)
    vol_hi, vol_lo = split_const(volume)
    onto_hi, onto_lo = split_const(onto)
    off_hi, off_lo = split_const(off)
    lift_hi, lift_lo = split_const(lift)
    onto_main = np.concatenate([onto_hi, onto_hi], axis=0)
    off_main = np.concatenate(
        [
            np.concatenate([off_hi, off_lo], axis=2),
            np.concatenate([off_hi, np.zeros_like(off_lo)], axis=2),
        ],
        axis=1,
    )
    lift_main = np.concatenate([lift_hi, lift_hi], axis=1)
    spread = np.zeros((30, 64, 128), np.float32)
    for slab in range(30):
        spread[slab, slab, :SLOPE_AT] = 1.0
        spread[slab, 32 + slab, SLOPE_AT:] = 1.0
    inv_diag = np.zeros((1, 256), np.float32)
    inv_diag[0, :216] = 1.0 / stiff_diag
    traces = [m[:, at : at + 256] for m in (faces_hi, faces_lo) for at in (0, 256, 512)]
    traces += [m[:, at : at + 256] for m in (onto_main, onto_lo) for at in (0, 256)]
    spread = spread.reshape(5, 6, 64, 128).transpose(1, 2, 0, 3).reshape(6, 64, 640)
    return dict(
        traces=np.concatenate(traces, axis=0),
        volume=np.concatenate([vol_hi, vol_lo], axis=0),
        off_main=off_main,
        lift_main=lift_main,
        lift_lo=lift_lo,
        spread=spread.astype(BF),
        inv_diag=inv_diag,
    )


def dot(left, right):
    return lax.dot_general(left, right, (((1,), (0,)), ((), ())), preferred_element_type=F32)


def split(value):
    high = value.astype(BF)
    return high, (value - high.astype(F32)).astype(BF)


def lane_groups(elems):
    lane = lax.broadcasted_iota(jnp.int32, (elems, 128), 1)
    return lane < SLOPE_AT, lane < AGAIN_AT


def safe_inverse(size):
    return jnp.where(size > 0.0, 1.0 / jnp.maximum(size, 0.5), 0.0)


def write_tables(x, size, consts, pool, elems):
    slab = 6 * elems
    is_value, below_again = lane_groups(elems)
    is_slope = jnp.logical_and(below_again, jnp.logical_not(is_value))
    scale = jnp.where(is_slope, safe_inverse(size), 1.0)
    x_hi, x_lo = split(x)
    traces = consts["traces"]
    for pair in range(3):
        hi = traces[pair * 256 : (pair + 1) * 256, :]
        lo = traces[(pair + 3) * 256 : (pair + 4) * 256, :]
        both = dot(x_hi, hi) + dot(x_lo, hi) + dot(x_hi, lo)
        for part in range(2):
            direction = 2 * pair + part
            row = both[:, part * 128 : (part + 1) * 128] * scale
            pool[4 * slab + direction * elems : 4 * slab + (direction + 1) * elems, :] = row

    def quarters(direction):
        at = direction * elems
        row_hi, row_lo = split(pool[pl.ds(4 * slab + at, elems), :])
        both_rows = jnp.concatenate([row_hi, row_lo], axis=1)
        for pair in range(2):
            both = dot(both_rows, traces[(6 + pair) * 256 : (7 + pair) * 256, :])
            both = both + dot(row_hi, traces[2048 + pair * 128 : 2176 + pair * 128, :])
            pool[pl.ds(2 * pair * slab + at, elems), :] = both[:, :128]
            pool[pl.ds((2 * pair + 1) * slab + at, elems), :] = both[:, 128:]

    for direction in range(6):
        quarters(direction)


class Fetch:
    def __init__(self, names, sources, targets, sems):
        self.copies = {
            name: pltpu.make_async_copy(source, target, sems.at[i])
            for i, (name, source, target) in enumerate(zip(names, sources, targets))
        }

    def start(self):
        for copy in self.copies.values():
            copy.start()

    def wait(self, *names):
        for name in names:
            self.copies.pop(name).wait()


class View:
    def __init__(self, ref, base):
        self.ref = ref
        self.base = base

    def __getitem__(self, index):
        return self.ref[self.base + index]


def resolve_lists(packed, lists, first_row, result):
    for at in range(0, 32, 8):
        index = lists[at : at + 8, :]
        group = index >> 7
        lane = index & 127
        found = jnp.zeros((8, 128), jnp.int32)
        for row in range(packed.shape[0]):
            source = jnp.broadcast_to(packed[row : row + 1, :], (8, 128))
            taken = jnp.take_along_axis(source, lane, axis=1)
            found = jnp.where(group == row, taken, found)
        result[at : at + 8, :] = found & ((1 << PAIR_BITS) - 1)
        line = lax.broadcasted_iota(jnp.int32, (8, 128), 0) + at
        slot = lax.broadcasted_iota(jnp.int32, (8, 128), 1) + (line & 1) * 128
        here = (found >> PAIR_BITS) - 1 == first_row + (line >> 1)
        end = jnp.max(jnp.where(here, slot + 1, 0), axis=1, keepdims=True)
        result[32 + at : 40 + at, :] = jnp.broadcast_to(end, (8, 128))


def pack_rows(slots, info, pool, staging, outs, sems, capacity):
    copies = []
    for position, out in enumerate(outs):
        row = 2 * jnp.clip(info[0] + STEPS[position], 0, 2 * REACH)
        end = jnp.maximum(slots[32 + row, 0], slots[33 + row, 0])

        def chunk(k, carry, row=row, position=position):
            rows = []
            line = row + (k * PACK_UNROLL) // 128
            column = k * PACK_UNROLL % 128
            for u in range(PACK_UNROLL):
                rows.append(pool[pl.ds(slots[line, column + u], 1), :])
            for u in range(PACK_UNROLL):
                staging[pl.ds(position * capacity + k * PACK_UNROLL + u, 1), :] = rows[u]
            return carry

        lax.fori_loop(0, (end + PACK_UNROLL - 1) // PACK_UNROLL, chunk, 0)
        here = staging.at[position * capacity : (position + 1) * capacity, :]
        copies.append(pltpu.make_async_copy(here, out, sems.at[position]))
        copies[-1].start()
    for copy in copies:
        copy.wait()


FIRST_NAMES = ("traces",)
LAST_NAMES = ("off_main", "spread", "lift_main", "lift_lo")


def first_kernel(elems, capacity):
    def body(*refs):
        start, size_ref, packed, lists, info = refs[:5]
        consts = dict(zip(FIRST_NAMES, refs[5 : 5 + len(FIRST_NAMES)]))
        x_out, pool, slots, *rest = refs[5 + len(FIRST_NAMES) :]
        outs = rest[: 2 * REACH]
        staging, out_sems, resolved, sem = rest[2 * REACH :]
        resolve_lists(packed, lists, info[1], resolved)
        copy = pltpu.make_async_copy(resolved, slots, sem)
        copy.start()
        x = jnp.concatenate([start[...].T, jnp.zeros((elems, 40), F32)], axis=1)
        x_out[...] = x
        write_tables(x, size_ref[...], consts, pool, elems)
        copy.wait()
        pack_rows(slots, info, pool, staging, outs, out_sems, capacity)

    return body


def add_rows(flag, count, source, target, pool, sums):
    @pl.when(flag == 0)
    def _():
        def chunk(k, carry):
            base = k * UNROLL
            rows = []
            for u in range(UNROLL):
                rows.append(pool[pl.ds(source(base + u), 1), :])
            for u in range(UNROLL):
                sums[pl.ds(target(base + u), 1), :] = rows[u]
            return carry

        lax.fori_loop(0, (count + UNROLL - 1) // UNROLL, chunk, 0)

    @pl.when(flag != 0)
    def _():
        def one(r, carry):
            here = pl.ds(target(r), 1)
            sums[here, :] = sums[here, :] + pool[pl.ds(source(r), 1), :]
            return carry

        lax.fori_loop(0, count, one, 0)


def inner_kernel(elems, records, compact):
    table_rows = 30 * elems

    def body(*refs):
        if compact:
            x_ref, size_ref, pool, ints, recs, vol, sums, total, far_pairs, counts_out = refs
            far_pair = View(ints, 3 * records)
        else:
            x_ref, size_ref, pool, ints, far_pairs, vol, sums, total = refs
        table_row, local_rec, local_row = (View(ints, i * records) for i in range(3))
        if compact:
            row_iota = lax.broadcasted_iota(jnp.int32, (64, records), 0)
            slabs = recs[1:2, :]
            weight = recs[2:3, :].astype(F32)
            low = jnp.where(row_iota == slabs, 1.0, 0.0)
            high = jnp.where(row_iota - 32 == slabs, 1.0, 0.0) * weight
            kinds = (low + high).astype(BF)
            elem_iota = lax.broadcasted_iota(jnp.int32, (elems, records), 0)
            onehot = jnp.where(elem_iota == recs[0:1, :], 1.0, 0.0).astype(BF)
            counts = lax.dot_general(
                onehot, kinds, (((1,), (1,)), ((), ())), preferred_element_type=F32
            )
            counts_out[...] = counts
            paired = 2.0 * counts[:, :32] - counts[:, 32:]
            flag = jnp.where(jnp.max(paired) > 1.5, 1, 0)
        else:
            flag = far_pairs[records + UNROLL + 1]

        def clear(k, carry):
            at = pl.multiple_of(k * elems, elems)
            sums[pl.ds(at, elems), :] = jnp.zeros((elems, 128), F32)
            return carry

        lax.fori_loop(0, 30, clear, 0)
        sums[table_rows : table_rows + 8, :] = jnp.zeros((8, 128), F32)
        add_rows(
            flag,
            records,
            lambda r: table_row[local_rec[r]],
            lambda r: local_row[r],
            pool,
            sums,
        )
        x_hi, x_lo = split(x_ref[...])
        hi = vol[:256, :]
        volume = dot(x_hi, hi) + dot(x_lo, hi) + dot(x_hi, vol[256:, :])
        size = size_ref[...]
        total[...] = volume * jnp.concatenate([size, size], axis=1)
        if compact:

            def collect(k, count):
                pairs = [far_pair[k * 16 + u] for u in range(16)]
                for pair in pairs:
                    far_pairs[count] = pair
                    count = count + jnp.where(pair >= 0, 1, 0)
                return count

            count = lax.fori_loop(0, records // 16, collect, 0)
            for u in range(UNROLL):
                far_pairs[count + u] = table_rows
            far_pairs[records + UNROLL] = count
            far_pairs[records + UNROLL + 1] = flag

    return body


def outer_kernel(elems, capacity, records, step, last):
    slab = 6 * elems
    table_rows = 5 * slab
    const_names = LAST_NAMES if last else LAST_NAMES + FIRST_NAMES
    block_names = tuple("block%d" % i for i in range(2 * REACH))

    def body(*refs):
        x_ref, dirn_ref, rhs_ref, size_ref, counts_ref, pool, near, volume, inv_diag = refs[:9]
        scalars, far_pairs, slots, info = refs[9:13]
        received = refs[13 : 13 + 2 * REACH]
        at = 13 + 2 * REACH
        consts = dict(zip(const_names, refs[at : at + len(const_names)]))
        rest = refs[at + len(const_names) :]
        if last:
            earlier = rest[: ITERS - 1]
            sums, x_out, norm_out = rest[ITERS - 1 : ITERS + 2]
            rest = rest[ITERS + 2 :]
        else:
            sums, x_out, dirn_out, norm_out, pool = rest[:5]
            outs = rest[5 : 5 + 2 * REACH]
            rest = rest[5 + 2 * REACH :]
        blocks, total, sems, out_sems = rest
        fetch = Fetch(
            block_names,
            received,
            [blocks.at[i * capacity : (i + 1) * capacity, :] for i in range(2 * REACH)],
            sems,
        )
        fetch.start()
        size = size_ref[...]
        inverse = safe_inverse(size)
        fetch.wait(*block_names)
        add_rows(
            far_pairs[records + UNROLL + 1],
            far_pairs[records + UNROLL],
            lambda r: far_pairs[r] >> PAIR_BITS,
            lambda r: far_pairs[r] & ((1 << PAIR_BITS) - 1),
            blocks,
            sums,
        )
        size_wide = jnp.concatenate([size, size], axis=1)
        total[...] = volume[...]
        counts = counts_ref[...].astype(BF)
        is_value, below_again = lane_groups(elems)

        def direction_terms(direction):
            at = direction * elems
            acc = jnp.zeros((elems, 256), F32)
            spread = dot(counts, consts["spread"][direction])
            for sub in range(5):
                edge = size if sub == 4 else 0.5 * size
                area = -0.5 * edge * edge
                coef = jnp.where(is_value, edge, jnp.where(below_again, area, area * inverse))
                rows = pl.ds(sub * slab + at, elems)
                times = spread[:, sub * 128 : (sub + 1) * 128]
                term = coef * (pool[rows, :] * times - sums[rows, :])
                term_hi, term_lo = split(term)
                acc = acc + dot(
                    jnp.concatenate([term_hi, term_lo], axis=1), consts["off_main"][sub]
                )
            face = acc[:, :128] + acc[:, 128:]
            face_hi, face_lo = split(face)
            total[...] += dot(
                jnp.concatenate([face_hi, face_lo], axis=1), consts["lift_main"][direction]
            ) + dot(face_hi, consts["lift_lo"][direction])

        for direction in range(6):
            direction_terms(direction)
        rhs = jnp.concatenate([rhs_ref[...].T, jnp.zeros((elems, 40), F32)], axis=1)
        residual = jnp.where(size_wide > 0.0, rhs - total[...], 0.0)
        scaled = residual * (jnp.concatenate([inverse, inverse], axis=1) * inv_diag[...])

        def fold(product):
            part = jnp.sum(product.reshape(elems // 8, 8, 256), axis=0)
            return part[:, :128] + part[:, 128:]

        folded = (fold(residual * residual), fold(residual * scaled))
        if last:
            pieces = [n[at : at + 8, :] for n in earlier for at in (0, 8)] + list(folded)
            lane = lax.broadcasted_iota(jnp.int32, norm_out.shape, 1)
            row = jnp.zeros(norm_out.shape, F32)
            for i, piece in enumerate(pieces):
                row = jnp.where(lane == i, jnp.sum(piece), row)
            norm_out[...] = row
        else:
            norm_out[0:8, :] = folded[0]
            norm_out[8:16, :] = folded[1]
        dirn = scalars[2 * step + 1] * scaled
        if step > 0:
            dirn = scalars[2 * step] * dirn_ref[...] + dirn
        x_new = x_ref[...] + dirn
        if last:
            x_out[...] = x_new[:, :216].T
        else:
            x_out[...] = x_new
            dirn_out[...] = dirn
            write_tables(x_new, size, consts, pool, elems)
            pack_rows(slots, info, pool, blocks, outs, out_sems, capacity)

    return body


def on_device(
    rhs, start, spectrum_top, elem_code, rec_elem, rec_dir, rec_sub, rec_peer, rec_index, send_rec
):
    consts = build_constants()
    parts = lax.axis_size(AXIS)
    own = lax.axis_index(AXIS)
    elems = rhs.shape[1]
    records = rec_elem.shape[0]
    capacity = send_rec.shape[0] // parts
    slab = 6 * elems
    table_rows = 5 * slab

    size = jnp.broadcast_to((0.5 * elem_code.astype(F32))[:, None], (elems, 128))
    sub = jnp.minimum(rec_sub, 4)
    table_row = sub * slab + rec_dir * elems + rec_elem
    live = rec_sub < 5
    bound = rec_peer < 0
    local = jnp.logical_and(rec_peer == own, live)
    far = jnp.logical_and(jnp.logical_not(bound), rec_peer != own)
    far = jnp.logical_and(far, live)
    offset = own - rec_peer
    position = jnp.where(offset > 0, offset - 1, 2 * REACH + offset)
    far_row = jnp.clip(position, 0, 2 * REACH - 1) * capacity + rec_index
    far_pair = jnp.where(far, far_row * (1 << PAIR_BITS) + table_row, -1)
    local_rec = jnp.where(local, rec_index, 0)
    local_row = jnp.where(local, table_row, table_rows)
    kind = jnp.where(live, sub * 6 + rec_dir, 99)
    recs = jnp.stack([rec_elem, kind, jnp.where(bound, 2, 1)])
    first_row = jnp.clip(own - REACH, 0, parts - 1 - 2 * REACH)
    lists = lax.dynamic_slice(
        send_rec.reshape(parts, capacity), (first_row, 0), (2 * REACH + 1, capacity)
    )
    lists = jnp.pad(lists.reshape(-1, 128), ((0, 2), (0, 0)))
    packed = ((rec_peer + 1) * (1 << PAIR_BITS) + table_row).reshape(-1, 128)
    info = jnp.stack([own - first_row, first_row]).astype(jnp.int32)

    top_value = spectrum_top[0]
    bottom = top_value / BOTTOM_RATIO
    center = 0.5 * (top_value + bottom)
    radius = 0.5 * (top_value - bottom)
    sigma_ratio = center / radius
    rho_prev = 1.0 / sigma_ratio
    factors = [jnp.zeros((), F32), 1.0 / center]
    for _ in range(1, ITERS):
        rho_next = 1.0 / (2.0 * sigma_ratio - rho_prev)
        factors += [rho_next * rho_prev, 2.0 * rho_next / radius]
        rho_prev = rho_next
    factors = jnp.stack(factors)
    near_ints = jnp.concatenate([table_row, local_rec, local_row, far_pair])
    (size, packed, lists, info, near_ints, recs, factors, start) = lax.optimization_barrier(
        (size, packed, lists, info, near_ints, recs, factors, start)
    )

    vmem = pl.BlockSpec(memory_space=pltpu.VMEM)
    smem = pl.BlockSpec(memory_space=pltpu.SMEM)
    hbm = pl.BlockSpec(memory_space=pltpu.HBM)
    field = jax.ShapeDtypeStruct((elems, 256), F32)
    block = jax.ShapeDtypeStruct((capacity, 128), F32)
    table = jax.ShapeDtypeStruct((table_rows, 128), F32)
    table_more = jax.ShapeDtypeStruct((table_rows + 8, 128), F32)
    params = pltpu.CompilerParams(vmem_limit_bytes=VMEM_MIB << 20)
    small = pltpu.CompilerParams(vmem_limit_bytes=SMALL_MIB << 20)
    staging = pltpu.VMEM((2 * REACH * capacity, 128), F32)
    blocks_out = (block,) * (2 * REACH)
    nodes = rhs.shape[0]

    def pick(names):
        return [consts[n] for n in names]

    def sems(count):
        return pltpu.SemaphoreType.DMA((count,))

    x, pool, slots, *blocks = pl.pallas_call(
        first_kernel(elems, capacity),
        name="first_traces",
        out_shape=(field, table, jax.ShapeDtypeStruct((64, 128), jnp.int32)) + blocks_out,
        in_specs=[vmem] * 4 + [smem] + [vmem] * len(FIRST_NAMES),
        out_specs=(vmem, vmem, smem) + (hbm,) * (2 * REACH),
        scratch_shapes=[
            staging,
            sems(2 * REACH),
            pltpu.VMEM((64, 128), jnp.int32),
            pltpu.SemaphoreType.DMA,
        ],
        compiler_params=small,
    )(start, size, packed, lists, info, *pick(FIRST_NAMES))

    dirn = x
    norms = []
    for step in range(ITERS):
        last = step == ITERS - 1
        compact = step == 0
        received = [
            lax.ppermute(piece, AXIS, [(i, (i + by) % parts) for i in range(parts)])
            for piece, by in zip(blocks, STEPS)
        ]
        ints = jax.ShapeDtypeStruct((records + UNROLL + 2,), jnp.int32)
        results = pl.pallas_call(
            inner_kernel(elems, records, compact),
            name="inner_%d" % step,
            out_shape=(table_more, field)
            + ((ints, jax.ShapeDtypeStruct((elems, 64), F32)) if compact else ()),
            in_specs=[vmem] * 3 + [smem, vmem if compact else smem, vmem],
            out_specs=(vmem, vmem) + ((smem, vmem) if compact else ()),
            compiler_params=small,
            cost_estimate=pl.CostEstimate(
                flops=10**10, transcendentals=0, bytes_accessed=10**6
            ),
        )(
            x,
            size,
            pool,
            near_ints,
            recs if compact else far_list,
            consts["volume"],
        )
        near, volume = results[:2]
        if compact:
            far_list, counts = results[2:]
        norm_shape = jax.ShapeDtypeStruct((16, 128), F32)
        if last:
            shapes = (
                table_more,
                jax.ShapeDtypeStruct((nodes, elems), F32),
                jax.ShapeDtypeStruct((parts, 128), F32),
            )
            out_specs = (vmem,) * 3
        else:
            shapes = (table_more, field, field, norm_shape, table) + blocks_out
            out_specs = (vmem,) * 5 + (hbm,) * (2 * REACH)
        names = LAST_NAMES if last else LAST_NAMES + FIRST_NAMES
        results = pl.pallas_call(
            outer_kernel(elems, capacity, records, step, last),
            name="outer_%d" % step,
            out_shape=shapes,
            in_specs=[vmem] * 9
            + [smem] * 4
            + [hbm] * (2 * REACH)
            + [vmem] * (len(names) + (len(norms) if last else 0)),
            out_specs=out_specs,
            scratch_shapes=[
                staging,
                pltpu.VMEM((elems, 256), F32),
                sems(2 * REACH),
                sems(2 * REACH),
            ],
            input_output_aliases={6: 0} if last else {6: 0, 5: 4},
            compiler_params=params,
        )(
            x,
            dirn,
            rhs,
            size,
            counts,
            pool,
            near,
            volume,
            consts["inv_diag"],
            factors,
            far_list,
            slots,
            info,
            *received,
            *pick(names),
            *(norms if last else ()),
        )
        if last:
            _, answer, mine = results
        else:
            _, x, dirn, norm, pool, *blocks = results
            norms.append(norm)

    gathered = lax.all_to_all(mine, AXIS, 0, 0, tiled=True)
    total = jnp.sum(gathered, axis=0)[:6].reshape(3, 2)
    return (answer, 0.5 * jnp.log(total / (216.0 * elems * parts)))


def solution(mesh):
    split_spec = P(AXIS)
    in_specs = (P(None, AXIS), P(None, AXIS), P()) + (split_spec,) * 7
    out_specs = (P(None, AXIS), P())
    return jax.shard_map(
        on_device, mesh=mesh, in_specs=in_specs, out_specs=out_specs, check_vma=False
    )
```

```python
import functools
import math

import jax
import jax.numpy as jnp
import numpy as np
from jax import lax
from jax.experimental import pallas as pl
from jax.experimental.pallas import tpu as pltpu
from jax.sharding import PartitionSpec as P

ITERS = 3
REACH = 7
AXIS = "parts"
PENALTY = 36.0
BOTTOM_RATIO = 8.0
SLOPE_AT = 40
AGAIN_AT = 80
UNROLL = 32
PACK_UNROLL = 32
TOGETHER = 2


BF = jnp.bfloat16
F32 = jnp.float32
STEPS = list(range(1, REACH + 1)) + list(range(-REACH, 0))
VMEM_MIB = 10
SMALL_MIB = 10
PAIR_BITS = 14


def lobatto_tables():
    root_seven = math.sqrt(7.0)
    inner_root = math.sqrt(1.0 / 3.0 - 2.0 * root_seven / 21.0)
    outer_root = math.sqrt(1.0 / 3.0 + 2.0 * root_seven / 21.0)
    points = (np.array([-1.0, -outer_root, -inner_root, inner_root, outer_root, 1.0]) + 1.0) / 2.0
    weights = (
        np.array(
            [
                1.0 / 15.0,
                (14.0 - root_seven) / 30.0,
                (14.0 + root_seven) / 30.0,
                (14.0 + root_seven) / 30.0,
                (14.0 - root_seven) / 30.0,
                1.0 / 15.0,
            ]
        )
        / 2.0
    )
    barycentric = np.array(
        [1.0 / np.prod([points[j] - points[k] for k in range(6) if k != j]) for j in range(6)]
    )
    derivative = np.zeros((6, 6))
    for i in range(6):
        for j in range(6):
            if i != j:
                derivative[i, j] = barycentric[j] / barycentric[i] / (points[i] - points[j])
        derivative[i, i] = -np.sum(derivative[i])
    halves = np.zeros((2, 6, 6))
    for which_half in range(2):
        targets = (points + which_half) / 2.0
        for i in range(6):
            for j in range(6):
                halves[which_half, i, j] = np.prod(
                    [(targets[i] - points[k]) / (points[j] - points[k]) for k in range(6) if k != j]
                )
    column_sums = np.sum(derivative * derivative * weights[:, None], axis=0)
    stiff_diag = (
        column_sums[:, None, None] * weights[None, :, None] * weights[None, None, :]
        + weights[:, None, None] * column_sums[None, :, None] * weights[None, None, :]
        + weights[:, None, None] * weights[None, :, None] * column_sums[None, None, :]
    )
    return (weights, derivative, halves, stiff_diag.reshape(216))


def split_const(matrix):
    high = np.asarray(matrix, np.float32).astype(BF)
    low = (np.asarray(matrix, np.float64) - high.astype(np.float64)).astype(BF)
    return high, low


def build_constants():
    weights, derivative, halves, stiff_diag = lobatto_tables()
    eye = np.eye(6)
    faces = np.zeros((256, 6 * 128))
    lift = np.zeros((6, 128, 256))
    for direction in range(6):
        axis_index = direction // 2
        layer = 5 * (direction % 2)
        value_vec = eye[layer]
        slope_vec = (2.0 * (direction % 2) - 1.0) * derivative[layer]
        for vec, places, lift_at in (
            (value_vec, (0, AGAIN_AT), 0),
            (slope_vec, (SLOPE_AT,), SLOPE_AT),
        ):
            if axis_index == 0:
                block = np.einsum("i,jp,kq->ijkpq", vec, eye, eye)
            elif axis_index == 1:
                block = np.einsum("j,ip,kq->ijkpq", vec, eye, eye)
            else:
                block = np.einsum("k,ip,jq->ijkpq", vec, eye, eye)
            block = block.reshape(216, 36)
            for place in places:
                faces[:216, direction * 128 + place : direction * 128 + place + 36] = block
            lift[direction, lift_at : lift_at + 36, :216] = block.T
    stiff = derivative.T @ np.diag(weights) @ derivative
    mass = np.diag(weights)
    volume = np.zeros((256, 256))
    volume[:216, :216] = (
        np.kron(stiff, np.kron(mass, mass))
        + np.kron(mass, np.kron(stiff, mass))
        + np.kron(mass, np.kron(mass, stiff))
    )
    onto = np.zeros((128, 4 * 128))
    off = np.zeros((5, 128, 128))
    face_weight = np.kron(weights, weights)
    for sub in range(5):
        if sub < 4:
            mortar = np.kron(halves[sub % 2], halves[sub // 2]).T
            onto[0:36, sub * 128 : sub * 128 + 36] = mortar
            onto[0:36, sub * 128 + AGAIN_AT : sub * 128 + AGAIN_AT + 36] = mortar
            onto[SLOPE_AT : SLOPE_AT + 36, sub * 128 + SLOPE_AT : sub * 128 + SLOPE_AT + 36] = mortar
        else:
            mortar = np.eye(36)
        back = face_weight[:, None] * mortar.T
        off[sub, 0:36, 0:36] = PENALTY * back
        off[sub, SLOPE_AT : SLOPE_AT + 36, 0:36] = back
        off[sub, AGAIN_AT : AGAIN_AT + 36, SLOPE_AT : SLOPE_AT + 36] = back
    faces_hi, faces_lo = split_const(faces)
    vol_hi, vol_lo = split_const(volume)
    onto_hi, onto_lo = split_const(onto)
    off_hi, off_lo = split_const(off)
    lift_hi, lift_lo = split_const(lift)
    onto_main = np.concatenate([onto_hi, onto_hi], axis=0)
    off_main = np.concatenate(
        [
            np.concatenate([off_hi, off_lo], axis=2),
            np.concatenate([off_hi, np.zeros_like(off_lo)], axis=2),
        ],
        axis=1,
    )
    lift_main = np.concatenate([lift_hi, lift_hi], axis=1)
    spread = np.zeros((30, 64, 128), np.float32)
    for slab in range(30):
        spread[slab, slab, :SLOPE_AT] = 1.0
        spread[slab, 32 + slab, SLOPE_AT:] = 1.0
    inv_diag = np.zeros((1, 256), np.float32)
    inv_diag[0, :216] = 1.0 / stiff_diag
    traces = [m[:, at : at + 256] for m in (faces_hi, faces_lo) for at in (0, 256, 512)]
    traces += [m[:, at : at + 256] for m in (onto_main, onto_lo) for at in (0, 256)]
    spread = spread.reshape(5, 6, 64, 128).transpose(1, 2, 0, 3).reshape(6, 64, 640)
    return dict(
        traces=np.concatenate(traces, axis=0),
        volume=np.concatenate([vol_hi, vol_lo], axis=0),
        off_main=off_main,
        lift_main=lift_main,
        lift_lo=lift_lo,
        spread=spread.astype(BF),
        inv_diag=inv_diag,
    )


def dot(left, right):
    return lax.dot_general(left, right, (((1,), (0,)), ((), ())), preferred_element_type=F32)


def split(value):
    high = value.astype(BF)
    return high, (value - high.astype(F32)).astype(BF)


def lane_groups(elems):
    lane = lax.broadcasted_iota(jnp.int32, (elems, 128), 1)
    return lane < SLOPE_AT, lane < AGAIN_AT


def safe_inverse(size):
    return jnp.where(size > 0.0, 1.0 / jnp.maximum(size, 0.5), 0.0)


def each_direction(work):
    def several(k, carry):
        for side in range(TOGETHER):
            work(TOGETHER * k + side)
        return carry

    lax.fori_loop(0, 6 // TOGETHER, several, 0)


def write_tables(x, size, consts, pool, elems):
    slab = 6 * elems
    is_value, below_again = lane_groups(elems)
    is_slope = jnp.logical_and(below_again, jnp.logical_not(is_value))
    scale = jnp.where(is_slope, safe_inverse(size), 1.0)
    x_hi, x_lo = split(x)
    traces = consts["traces"]
    for pair in range(3):
        hi = traces[pair * 256 : (pair + 1) * 256, :]
        lo = traces[(pair + 3) * 256 : (pair + 4) * 256, :]
        both = dot(x_hi, hi) + dot(x_lo, hi) + dot(x_hi, lo)
        for part in range(2):
            direction = 2 * pair + part
            row = both[:, part * 128 : (part + 1) * 128] * scale
            pool[4 * slab + direction * elems : 4 * slab + (direction + 1) * elems, :] = row

    def quarters(direction):
        at = pl.multiple_of(direction * elems, elems)
        row_hi, row_lo = split(pool[pl.ds(4 * slab + at, elems), :])
        both_rows = jnp.concatenate([row_hi, row_lo], axis=1)
        for pair in range(2):
            both = dot(both_rows, traces[(6 + pair) * 256 : (7 + pair) * 256, :])
            both = both + dot(row_hi, traces[2048 + pair * 128 : 2176 + pair * 128, :])
            pool[pl.ds(2 * pair * slab + at, elems), :] = both[:, :128]
            pool[pl.ds((2 * pair + 1) * slab + at, elems), :] = both[:, 128:]

    each_direction(quarters)


class Fetch:
    def __init__(self, names, sources, targets, sems):
        self.copies = {
            name: pltpu.make_async_copy(source, target, sems.at[i])
            for i, (name, source, target) in enumerate(zip(names, sources, targets))
        }

    def start(self):
        for copy in self.copies.values():
            copy.start()

    def wait(self, *names):
        for name in names:
            self.copies.pop(name).wait()


class View:
    def __init__(self, ref, base):
        self.ref = ref
        self.base = base

    def __getitem__(self, index):
        return self.ref[self.base + index]


def resolve_lists(packed, lists, first_row, result):
    for at in range(0, 32, 8):
        index = lists[at : at + 8, :]
        group = index >> 7
        lane = index & 127
        found = jnp.zeros((8, 128), jnp.int32)
        for row in range(packed.shape[0]):
            source = jnp.broadcast_to(packed[row : row + 1, :], (8, 128))
            taken = jnp.take_along_axis(source, lane, axis=1)
            found = jnp.where(group == row, taken, found)
        result[at : at + 8, :] = found & ((1 << PAIR_BITS) - 1)
        line = lax.broadcasted_iota(jnp.int32, (8, 128), 0) + at
        slot = lax.broadcasted_iota(jnp.int32, (8, 128), 1) + (line & 1) * 128
        here = (found >> PAIR_BITS) - 1 == first_row + (line >> 1)
        end = jnp.max(jnp.where(here, slot + 1, 0), axis=1, keepdims=True)
        result[32 + at : 40 + at, :] = jnp.broadcast_to(end, (8, 128))


def pack_rows(slots, info, pool, staging, outs, sems, capacity):
    copies = []
    for position, out in enumerate(outs):
        row = 2 * jnp.clip(info[0] + STEPS[position], 0, 2 * REACH)
        end = jnp.maximum(slots[32 + row, 0], slots[33 + row, 0])

        def chunk(k, carry, row=row, position=position):
            rows = []
            line = row + (k * PACK_UNROLL) // 128
            column = k * PACK_UNROLL % 128
            for u in range(PACK_UNROLL):
                rows.append(pool[pl.ds(slots[line, column + u], 1), :])
            for u in range(PACK_UNROLL):
                staging[pl.ds(position * capacity + k * PACK_UNROLL + u, 1), :] = rows[u]
            return carry

        lax.fori_loop(0, (end + PACK_UNROLL - 1) // PACK_UNROLL, chunk, 0)
        here = staging.at[position * capacity : (position + 1) * capacity, :]
        copies.append(pltpu.make_async_copy(here, out, sems.at[position]))
        copies[-1].start()
    for copy in copies:
        copy.wait()


FIRST_NAMES = ("traces",)
LAST_NAMES = ("off_main", "spread", "lift_main", "lift_lo")


def first_kernel(elems, capacity):
    def body(*refs):
        start, size_ref, packed, lists, info = refs[:5]
        consts = dict(zip(FIRST_NAMES, refs[5 : 5 + len(FIRST_NAMES)]))
        x_out, pool, slots, *rest = refs[5 + len(FIRST_NAMES) :]
        outs = rest[: 2 * REACH]
        staging, out_sems, resolved, sem = rest[2 * REACH :]
        resolve_lists(packed, lists, info[1], resolved)
        copy = pltpu.make_async_copy(resolved, slots, sem)
        copy.start()
        x = jnp.concatenate([start[...].T, jnp.zeros((elems, 40), F32)], axis=1)
        x_out[...] = x
        write_tables(x, size_ref[...], consts, pool, elems)
        copy.wait()
        pack_rows(slots, info, pool, staging, outs, out_sems, capacity)

    return body


def compact_pairs(pairs, ranks, places, result, fill):
    lines = pairs.shape[0]
    flags = jnp.where(pairs[...] >= 0, 1.0, 0.0)
    columns = jnp.concatenate([flags, jnp.zeros((32 - lines, 128), F32)], axis=0).T.astype(BF)
    row = lax.broadcasted_iota(jnp.int32, (128, 128), 0)
    column = lax.broadcasted_iota(jnp.int32, (128, 128), 1)
    within = dot(jnp.where(row >= column, 1.0, 0.0).astype(BF), columns)
    earlier = jnp.where(row < column, 1.0, 0.0)[:32, :32].astype(BF)
    totals = jnp.broadcast_to(within[127:128, :], (8, 32)).astype(BF)
    before = dot(totals, earlier)[0:1, :]
    rank = within + before
    for line in range(lines):
        ranks[line * 128 : (line + 1) * 128, :] = jnp.broadcast_to(
            rank[:, line : line + 1], (128, 128)
        )
    count = jnp.sum(flags).astype(jnp.int32)
    places[...] = jnp.full(places.shape, float(lines * 128), F32)
    lane = lax.broadcasted_iota(jnp.int32, (8, 128), 1)

    def place(k, carry):
        target = (lane + k * 128).astype(F32)
        total = jnp.zeros((8, 128), F32)
        for at in range(0, lines * 128, 8):
            total = total + jnp.where(ranks[at : at + 8, :] <= target, 1.0, 0.0)
        places[pl.ds(k, 1), :] = jnp.sum(total, axis=0, keepdims=True)
        return carry

    lax.fori_loop(0, (count + 127) // 128, place, 0)
    for at in range(0, lines, 8):
        index = places[at : at + 8, :].astype(jnp.int32)
        found = jnp.full((8, 128), fill, jnp.int32)
        for line in range(lines):
            source = jnp.broadcast_to(pairs[line : line + 1, :], (8, 128))
            taken = jnp.take_along_axis(source, index & 127, axis=1)
            found = jnp.where((index >> 7) == line, taken, found)
        result[at : at + 8, :] = found
    return count


def add_rows(flag, count, source, target, pool, sums):
    @pl.when(flag == 0)
    def _():
        def chunk(k, carry):
            base = k * UNROLL
            rows = []
            for u in range(UNROLL):
                rows.append(pool[pl.ds(source(base, u), 1), :])
            for u in range(UNROLL):
                sums[pl.ds(target(base, u), 1), :] = rows[u]
            return carry

        lax.fori_loop(0, (count + UNROLL - 1) // UNROLL, chunk, 0)

    @pl.when(flag != 0)
    def _():
        def one(r, carry):
            here = pl.ds(target(r, 0), 1)
            sums[here, :] = sums[here, :] + pool[pl.ds(source(r, 0), 1), :]
            return carry

        lax.fori_loop(0, count, one, 0)


def inner_kernel(elems, records, compact):
    table_rows = 30 * elems

    def body(*refs):
        if compact:
            x_ref, size_ref, pool, ints, recs, far_pair, vol = refs[:7]
            sums, total, far_pairs, meta, counts_out, ranks, places, packed, sem = refs[7:]
            count = compact_pairs(far_pair, ranks, places, packed, table_rows)
            meta[0] = count
            copy = pltpu.make_async_copy(packed, far_pairs, sem)
            copy.start()
        else:
            x_ref, size_ref, pool, ints, meta, vol, sums, total = refs
        table_row, local_rec, local_row = (View(ints, i * records) for i in range(3))
        if compact:
            row_iota = lax.broadcasted_iota(jnp.int32, (64, records), 0)
            slabs = recs[1:2, :]
            weight = recs[2:3, :].astype(F32)
            low = jnp.where(row_iota == slabs, 1.0, 0.0)
            high = jnp.where(row_iota - 32 == slabs, 1.0, 0.0) * weight
            kinds = (low + high).astype(BF)
            elem_iota = lax.broadcasted_iota(jnp.int32, (elems, records), 0)
            onehot = jnp.where(elem_iota == recs[0:1, :], 1.0, 0.0).astype(BF)
            counts = lax.dot_general(
                onehot, kinds, (((1,), (1,)), ((), ())), preferred_element_type=F32
            )
            counts_out[...] = counts
            paired = 2.0 * counts[:, :32] - counts[:, 32:]
            flag = jnp.where(jnp.max(paired) > 1.5, 1, 0)
            meta[1] = flag
        else:
            flag = meta[1]

        def clear(k, carry):
            at = pl.multiple_of(k * elems, elems)
            sums[pl.ds(at, elems), :] = jnp.zeros((elems, 128), F32)
            return carry

        lax.fori_loop(0, 30, clear, 0)
        sums[table_rows : table_rows + 8, :] = jnp.zeros((8, 128), F32)
        add_rows(
            flag,
            records,
            lambda base, u: table_row[local_rec[base + u]],
            lambda base, u: local_row[base + u],
            pool,
            sums,
        )
        x_hi, x_lo = split(x_ref[...])
        hi = vol[:256, :]
        volume = dot(x_hi, hi) + dot(x_lo, hi) + dot(x_hi, vol[256:, :])
        size = size_ref[...]
        total[...] = volume * jnp.concatenate([size, size], axis=1)
        if compact:
            copy.wait()

    return body


def outer_kernel(elems, capacity, records, step, last):
    slab = 6 * elems
    table_rows = 5 * slab
    const_names = LAST_NAMES if last else LAST_NAMES + FIRST_NAMES
    block_names = tuple("block%d" % i for i in range(2 * REACH))

    def body(*refs):
        x_ref, dirn_ref, rhs_ref, size_ref, counts_ref, pool, near, volume, inv_diag = refs[:9]
        scalars, far_pairs, meta, slots, info = refs[9:14]
        received = refs[14 : 14 + 2 * REACH]
        at = 14 + 2 * REACH
        consts = dict(zip(const_names, refs[at : at + len(const_names)]))
        rest = refs[at + len(const_names) :]
        if last:
            earlier = rest[: ITERS - 1]
            sums, x_out, norm_out = rest[ITERS - 1 : ITERS + 2]
            rest = rest[ITERS + 2 :]
        else:
            sums, x_out, dirn_out, norm_out, pool = rest[:5]
            outs = rest[5 : 5 + 2 * REACH]
            rest = rest[5 + 2 * REACH :]
        blocks, total, sems, out_sems = rest
        fetch = Fetch(
            block_names,
            received,
            [blocks.at[i * capacity : (i + 1) * capacity, :] for i in range(2 * REACH)],
            sems,
        )
        fetch.start()
        size = size_ref[...]
        inverse = safe_inverse(size)
        fetch.wait(*block_names)
        add_rows(
            meta[1],
            meta[0],
            lambda base, u: far_pairs[base >> 7, (base & 127) + u] >> PAIR_BITS,
            lambda base, u: far_pairs[base >> 7, (base & 127) + u] & ((1 << PAIR_BITS) - 1),
            blocks,
            sums,
        )
        size_wide = jnp.concatenate([size, size], axis=1)
        total[...] = volume[...]
        counts = counts_ref[...].astype(BF)
        is_value, below_again = lane_groups(elems)

        def direction_terms(direction):
            at = pl.multiple_of(direction * elems, elems)
            acc = jnp.zeros((elems, 256), F32)
            spread = dot(counts, consts["spread"][direction])
            for sub in range(5):
                edge = size if sub == 4 else 0.5 * size
                area = -0.5 * edge * edge
                coef = jnp.where(is_value, edge, jnp.where(below_again, area, area * inverse))
                rows = pl.ds(sub * slab + at, elems)
                times = spread[:, sub * 128 : (sub + 1) * 128]
                term = coef * (pool[rows, :] * times - sums[rows, :])
                term_hi, term_lo = split(term)
                acc = acc + dot(
                    jnp.concatenate([term_hi, term_lo], axis=1), consts["off_main"][sub]
                )
            face = acc[:, :128] + acc[:, 128:]
            face_hi, face_lo = split(face)
            total[...] += dot(
                jnp.concatenate([face_hi, face_lo], axis=1), consts["lift_main"][direction]
            ) + dot(face_hi, consts["lift_lo"][direction])

        each_direction(direction_terms)
        rhs = jnp.concatenate([rhs_ref[...].T, jnp.zeros((elems, 40), F32)], axis=1)
        residual = jnp.where(size_wide > 0.0, rhs - total[...], 0.0)
        scaled = residual * (jnp.concatenate([inverse, inverse], axis=1) * inv_diag[...])

        def fold(product):
            part = jnp.sum(product.reshape(elems // 8, 8, 256), axis=0)
            return part[:, :128] + part[:, 128:]

        folded = (fold(residual * residual), fold(residual * scaled))
        if last:
            pieces = [n[at : at + 8, :] for n in earlier for at in (0, 8)] + list(folded)
            lane = lax.broadcasted_iota(jnp.int32, norm_out.shape, 1)
            row = jnp.zeros(norm_out.shape, F32)
            for i, piece in enumerate(pieces):
                row = jnp.where(lane == i, jnp.sum(piece), row)
            norm_out[...] = row
        else:
            norm_out[0:8, :] = folded[0]
            norm_out[8:16, :] = folded[1]
        dirn = scalars[2 * step + 1] * scaled
        if step > 0:
            dirn = scalars[2 * step] * dirn_ref[...] + dirn
        x_new = x_ref[...] + dirn
        if last:
            x_out[...] = x_new[:, :216].T
        else:
            x_out[...] = x_new
            dirn_out[...] = dirn
            write_tables(x_new, size, consts, pool, elems)
            pack_rows(slots, info, pool, blocks, outs, out_sems, capacity)

    return body


def on_device(
    rhs, start, spectrum_top, elem_code, rec_elem, rec_dir, rec_sub, rec_peer, rec_index, send_rec
):
    consts = build_constants()
    parts = lax.axis_size(AXIS)
    own = lax.axis_index(AXIS)
    elems = rhs.shape[1]
    records = rec_elem.shape[0]
    capacity = send_rec.shape[0] // parts
    slab = 6 * elems
    table_rows = 5 * slab

    size = jnp.broadcast_to((0.5 * elem_code.astype(F32))[:, None], (elems, 128))
    sub = jnp.minimum(rec_sub, 4)
    table_row = sub * slab + rec_dir * elems + rec_elem
    live = rec_sub < 5
    bound = rec_peer < 0
    local = jnp.logical_and(rec_peer == own, live)
    far = jnp.logical_and(jnp.logical_not(bound), rec_peer != own)
    far = jnp.logical_and(far, live)
    offset = own - rec_peer
    position = jnp.where(offset > 0, offset - 1, 2 * REACH + offset)
    far_row = jnp.clip(position, 0, 2 * REACH - 1) * capacity + rec_index
    far_pair = jnp.where(far, far_row * (1 << PAIR_BITS) + table_row, -1)
    local_rec = jnp.where(local, rec_index, 0)
    local_row = jnp.where(local, table_row, table_rows)
    kind = jnp.where(live, sub * 6 + rec_dir, 99)
    recs = jnp.stack([rec_elem, kind, jnp.where(bound, 2, 1)])
    first_row = jnp.clip(own - REACH, 0, parts - 1 - 2 * REACH)
    lists = lax.dynamic_slice(
        send_rec.reshape(parts, capacity), (first_row, 0), (2 * REACH + 1, capacity)
    )
    lists = jnp.pad(lists.reshape(-1, 128), ((0, 2), (0, 0)))
    packed = ((rec_peer + 1) * (1 << PAIR_BITS) + table_row).reshape(-1, 128)
    info = jnp.stack([own - first_row, first_row]).astype(jnp.int32)

    top_value = spectrum_top[0]
    bottom = top_value / BOTTOM_RATIO
    center = 0.5 * (top_value + bottom)
    radius = 0.5 * (top_value - bottom)
    sigma_ratio = center / radius
    rho_prev = 1.0 / sigma_ratio
    factors = [jnp.zeros((), F32), 1.0 / center]
    for _ in range(1, ITERS):
        rho_next = 1.0 / (2.0 * sigma_ratio - rho_prev)
        factors += [rho_next * rho_prev, 2.0 * rho_next / radius]
        rho_prev = rho_next
    factors = jnp.stack(factors)
    near_ints = jnp.concatenate([table_row, local_rec, local_row])
    far_pair = far_pair.reshape(-1, 128)
    (size, packed, lists, info, near_ints, far_pair, recs, factors, start) = (
        lax.optimization_barrier(
            (size, packed, lists, info, near_ints, far_pair, recs, factors, start)
        )
    )

    vmem = pl.BlockSpec(memory_space=pltpu.VMEM)
    smem = pl.BlockSpec(memory_space=pltpu.SMEM)
    hbm = pl.BlockSpec(memory_space=pltpu.HBM)
    field = jax.ShapeDtypeStruct((elems, 256), F32)
    block = jax.ShapeDtypeStruct((capacity, 128), F32)
    table = jax.ShapeDtypeStruct((table_rows, 128), F32)
    table_more = jax.ShapeDtypeStruct((table_rows + 8, 128), F32)
    params = pltpu.CompilerParams(vmem_limit_bytes=VMEM_MIB << 20)
    small = pltpu.CompilerParams(vmem_limit_bytes=SMALL_MIB << 20)
    staging = pltpu.VMEM((2 * REACH * capacity, 128), F32)
    blocks_out = (block,) * (2 * REACH)
    nodes = rhs.shape[0]

    def pick(names):
        return [consts[n] for n in names]

    def sems(count):
        return pltpu.SemaphoreType.DMA((count,))

    x, pool, slots, *blocks = pl.pallas_call(
        first_kernel(elems, capacity),
        name="first_traces",
        out_shape=(field, table, jax.ShapeDtypeStruct((64, 128), jnp.int32)) + blocks_out,
        in_specs=[vmem] * 4 + [smem] + [vmem] * len(FIRST_NAMES),
        out_specs=(vmem, vmem, smem) + (hbm,) * (2 * REACH),
        scratch_shapes=[
            staging,
            sems(2 * REACH),
            pltpu.VMEM((64, 128), jnp.int32),
            pltpu.SemaphoreType.DMA,
        ],
        compiler_params=small,
    )(start, size, packed, lists, info, *pick(FIRST_NAMES))

    dirn = x
    norms = []
    for step in range(ITERS):
        last = step == ITERS - 1
        compact = step == 0
        received = [
            lax.ppermute(piece, AXIS, [(i, (i + by) % parts) for i in range(parts)])
            for piece, by in zip(blocks, STEPS)
        ]
        lines = records // 128
        pair_lines = jax.ShapeDtypeStruct((lines, 128), jnp.int32)
        results = pl.pallas_call(
            inner_kernel(elems, records, compact),
            name="inner_%d" % step,
            out_shape=(table_more, field)
            + (
                (
                    pair_lines,
                    jax.ShapeDtypeStruct((2,), jnp.int32),
                    jax.ShapeDtypeStruct((elems, 64), F32),
                )
                if compact
                else ()
            ),
            in_specs=[vmem] * 3 + [smem] + ([vmem, vmem] if compact else [smem]) + [vmem],
            out_specs=(vmem, vmem) + ((smem, smem, vmem) if compact else ()),
            scratch_shapes=[
                pltpu.VMEM((records, 128), F32),
                pltpu.VMEM((lines, 128), F32),
                pltpu.VMEM((lines, 128), jnp.int32),
                pltpu.SemaphoreType.DMA,
            ]
            if compact
            else [],
            compiler_params=small,
            cost_estimate=pl.CostEstimate(
                flops=10**10, transcendentals=0, bytes_accessed=10**6
            ),
        )(
            x,
            size,
            pool,
            near_ints,
            *((recs, far_pair) if compact else (meta,)),
            consts["volume"],
        )
        near, volume = results[:2]
        if compact:
            far_list, meta, counts = results[2:]
        norm_shape = jax.ShapeDtypeStruct((16, 128), F32)
        if last:
            shapes = (
                table_more,
                jax.ShapeDtypeStruct((nodes, elems), F32),
                jax.ShapeDtypeStruct((parts, 128), F32),
            )
            out_specs = (vmem,) * 3
        else:
            shapes = (table_more, field, field, norm_shape, table) + blocks_out
            out_specs = (vmem,) * 5 + (hbm,) * (2 * REACH)
        names = LAST_NAMES if last else LAST_NAMES + FIRST_NAMES
        results = pl.pallas_call(
            outer_kernel(elems, capacity, records, step, last),
            name="outer_%d" % step,
            out_shape=shapes,
            in_specs=[vmem] * 9
            + [smem] * 5
            + [hbm] * (2 * REACH)
            + [vmem] * (len(names) + (len(norms) if last else 0)),
            out_specs=out_specs,
            scratch_shapes=[
                staging,
                pltpu.VMEM((elems, 256), F32),
                sems(2 * REACH),
                sems(2 * REACH),
            ],
            input_output_aliases={6: 0} if last else {6: 0, 5: 4},
            compiler_params=params,
        )(
            x,
            dirn,
            rhs,
            size,
            counts,
            pool,
            near,
            volume,
            consts["inv_diag"],
            factors,
            far_list,
            meta,
            slots,
            info,
            *received,
            *pick(names),
            *(norms if last else ()),
        )
        if last:
            _, answer, mine = results
        else:
            _, x, dirn, norm, pool, *blocks = results
            norms.append(norm)

    gathered = lax.all_to_all(mine, AXIS, 0, 0, tiled=True)
    total = jnp.sum(gathered, axis=0)[:6].reshape(3, 2)
    return (answer, 0.5 * jnp.log(total / (216.0 * elems * parts)))


def solution(mesh):
    split_spec = P(AXIS)
    in_specs = (P(None, AXIS), P(None, AXIS), P()) + (split_spec,) * 7
    out_specs = (P(None, AXIS), P())
    return jax.shard_map(
        on_device, mesh=mesh, in_specs=in_specs, out_specs=out_specs, check_vma=False
    )
```

```python
import functools
import math

import jax
import jax.numpy as jnp
import numpy as np
from jax import lax
from jax.experimental import pallas as pl
from jax.experimental.pallas import tpu as pltpu
from jax.sharding import PartitionSpec as P

ITERS = 3
REACH = 7
AXIS = "parts"
PENALTY = 36.0
BOTTOM_RATIO = 8.0
SLOPE_AT = 40
AGAIN_AT = 80
UNROLL = 32
PACK_UNROLL = 32
TOGETHER = 2


BF = jnp.bfloat16
F32 = jnp.float32
STEPS = list(range(1, REACH + 1)) + list(range(-REACH, 0))
VMEM_MIB = 10
SMALL_MIB = 10
PAIR_BITS = 14


def lobatto_tables():
    root_seven = math.sqrt(7.0)
    inner_root = math.sqrt(1.0 / 3.0 - 2.0 * root_seven / 21.0)
    outer_root = math.sqrt(1.0 / 3.0 + 2.0 * root_seven / 21.0)
    points = (np.array([-1.0, -outer_root, -inner_root, inner_root, outer_root, 1.0]) + 1.0) / 2.0
    weights = (
        np.array(
            [
                1.0 / 15.0,
                (14.0 - root_seven) / 30.0,
                (14.0 + root_seven) / 30.0,
                (14.0 + root_seven) / 30.0,
                (14.0 - root_seven) / 30.0,
                1.0 / 15.0,
            ]
        )
        / 2.0
    )
    barycentric = np.array(
        [1.0 / np.prod([points[j] - points[k] for k in range(6) if k != j]) for j in range(6)]
    )
    derivative = np.zeros((6, 6))
    for i in range(6):
        for j in range(6):
            if i != j:
                derivative[i, j] = barycentric[j] / barycentric[i] / (points[i] - points[j])
        derivative[i, i] = -np.sum(derivative[i])
    halves = np.zeros((2, 6, 6))
    for which_half in range(2):
        targets = (points + which_half) / 2.0
        for i in range(6):
            for j in range(6):
                halves[which_half, i, j] = np.prod(
                    [(targets[i] - points[k]) / (points[j] - points[k]) for k in range(6) if k != j]
                )
    column_sums = np.sum(derivative * derivative * weights[:, None], axis=0)
    stiff_diag = (
        column_sums[:, None, None] * weights[None, :, None] * weights[None, None, :]
        + weights[:, None, None] * column_sums[None, :, None] * weights[None, None, :]
        + weights[:, None, None] * weights[None, :, None] * column_sums[None, None, :]
    )
    return (weights, derivative, halves, stiff_diag.reshape(216))


def split_const(matrix):
    high = np.asarray(matrix, np.float32).astype(BF)
    low = (np.asarray(matrix, np.float64) - high.astype(np.float64)).astype(BF)
    return high, low


def three_products(high, low):
    result = np.zeros((256, high.shape[1]), BF)
    result[:AGAIN_AT] = high[:AGAIN_AT]
    result[AGAIN_AT : AGAIN_AT + 36] = low[:36]
    result[128 : 128 + AGAIN_AT] = high[:AGAIN_AT]
    result[128 + AGAIN_AT : 128 + AGAIN_AT + 36] = low[SLOPE_AT : SLOPE_AT + 36]
    return result


def build_constants():
    weights, derivative, halves, stiff_diag = lobatto_tables()
    eye = np.eye(6)
    faces = np.zeros((256, 6 * 128))
    lift = np.zeros((6, 128, 256))
    for direction in range(6):
        axis_index = direction // 2
        layer = 5 * (direction % 2)
        value_vec = eye[layer]
        slope_vec = (2.0 * (direction % 2) - 1.0) * derivative[layer]
        for vec, places, lift_at in (
            (value_vec, (0, AGAIN_AT), 0),
            (slope_vec, (SLOPE_AT,), SLOPE_AT),
        ):
            if axis_index == 0:
                block = np.einsum("i,jp,kq->ijkpq", vec, eye, eye)
            elif axis_index == 1:
                block = np.einsum("j,ip,kq->ijkpq", vec, eye, eye)
            else:
                block = np.einsum("k,ip,jq->ijkpq", vec, eye, eye)
            block = block.reshape(216, 36)
            for place in places:
                faces[:216, direction * 128 + place : direction * 128 + place + 36] = block
            lift[direction, lift_at : lift_at + 36, :216] = block.T
    stiff = derivative.T @ np.diag(weights) @ derivative
    mass = np.diag(weights)
    volume = np.zeros((256, 256))
    volume[:216, :216] = (
        np.kron(stiff, np.kron(mass, mass))
        + np.kron(mass, np.kron(stiff, mass))
        + np.kron(mass, np.kron(mass, stiff))
    )
    onto = np.zeros((128, 4 * 128))
    off = np.zeros((5, 128, 128))
    face_weight = np.kron(weights, weights)
    for sub in range(5):
        if sub < 4:
            mortar = np.kron(halves[sub % 2], halves[sub // 2]).T
            onto[0:36, sub * 128 : sub * 128 + 36] = mortar
            onto[0:36, sub * 128 + AGAIN_AT : sub * 128 + AGAIN_AT + 36] = mortar
            onto[SLOPE_AT : SLOPE_AT + 36, sub * 128 + SLOPE_AT : sub * 128 + SLOPE_AT + 36] = mortar
        else:
            mortar = np.eye(36)
        back = face_weight[:, None] * mortar.T
        off[sub, 0:36, 0:36] = PENALTY * back
        off[sub, SLOPE_AT : SLOPE_AT + 36, 0:36] = back
        off[sub, AGAIN_AT : AGAIN_AT + 36, SLOPE_AT : SLOPE_AT + 36] = back
        off[sub, :, AGAIN_AT : AGAIN_AT + 36] = off[sub, :, 0:36]
    faces_hi, faces_lo = split_const(faces)
    vol_hi, vol_lo = split_const(volume)
    onto_hi, onto_lo = split_const(onto)
    off_hi, off_lo = split_const(off)
    lift_hi, lift_lo = split_const(lift)
    onto_main = three_products(onto_hi, onto_lo)
    off_main = np.concatenate(
        [
            np.concatenate([off_hi, off_lo], axis=2),
            np.concatenate([off_hi, np.zeros_like(off_lo)], axis=2),
        ],
        axis=1,
    )
    lift_main = np.stack([three_products(lift_hi[d], lift_lo[d]) for d in range(6)])
    spread = np.zeros((30, 64, 128), np.float32)
    for slab in range(30):
        spread[slab, slab, :SLOPE_AT] = 1.0
        spread[slab, 32 + slab, SLOPE_AT:] = 1.0
    inv_diag = np.zeros((1, 256), np.float32)
    inv_diag[0, :216] = 1.0 / stiff_diag
    traces = [m[:, at : at + 256] for m in (faces_hi, faces_lo) for at in (0, 256, 512)]
    traces += [onto_main[:, at : at + 256] for at in (0, 256)]
    spread = spread.reshape(5, 6, 64, 128).transpose(1, 2, 0, 3).reshape(6, 64, 640)
    return dict(
        traces=np.concatenate(traces, axis=0),
        volume=np.concatenate([vol_hi, vol_lo], axis=0),
        off_main=off_main,
        lift_main=lift_main,
        spread=spread.astype(BF),
        inv_diag=inv_diag,
    )


def dot(left, right):
    return lax.dot_general(left, right, (((1,), (0,)), ((), ())), preferred_element_type=F32)


def split(value):
    high = value.astype(BF)
    return high, (value - high.astype(F32)).astype(BF)


def rows_of_three(row):
    high = row.astype(BF)
    high_wide = high.astype(F32)
    lane = lax.broadcasted_iota(jnp.int32, row.shape, 1)
    moved = pltpu.roll(high_wide, AGAIN_AT - SLOPE_AT, axis=1)
    rest = jnp.where(lane < AGAIN_AT, row - high_wide, moved)
    return jnp.concatenate([high, rest.astype(BF)], axis=1)


def lane_groups(elems):
    lane = lax.broadcasted_iota(jnp.int32, (elems, 128), 1)
    return lane < SLOPE_AT, lane < AGAIN_AT


def safe_inverse(size):
    return jnp.where(size > 0.0, 1.0 / jnp.maximum(size, 0.5), 0.0)


def each_direction(work):
    def several(k, carry):
        for side in range(TOGETHER):
            work(TOGETHER * k + side)
        return carry

    lax.fori_loop(0, 6 // TOGETHER, several, 0)


def write_tables(x, size, consts, pool, elems):
    slab = 6 * elems
    is_value, below_again = lane_groups(elems)
    is_slope = jnp.logical_and(below_again, jnp.logical_not(is_value))
    scale = jnp.where(is_slope, safe_inverse(size), 1.0)
    x_hi, x_lo = split(x)
    traces = consts["traces"]
    for pair in range(3):
        hi = traces[pair * 256 : (pair + 1) * 256, :]
        lo = traces[(pair + 3) * 256 : (pair + 4) * 256, :]
        both = dot(x_hi, hi) + dot(x_lo, hi) + dot(x_hi, lo)
        for part in range(2):
            direction = 2 * pair + part
            row = both[:, part * 128 : (part + 1) * 128] * scale
            pool[4 * slab + direction * elems : 4 * slab + (direction + 1) * elems, :] = row

    def quarters(direction):
        at = pl.multiple_of(direction * elems, elems)
        both_rows = rows_of_three(pool[pl.ds(4 * slab + at, elems), :])
        for pair in range(2):
            both = dot(both_rows, traces[(6 + pair) * 256 : (7 + pair) * 256, :])
            pool[pl.ds(2 * pair * slab + at, elems), :] = both[:, :128]
            pool[pl.ds((2 * pair + 1) * slab + at, elems), :] = both[:, 128:]

    each_direction(quarters)


class Fetch:
    def __init__(self, names, sources, targets, sems):
        self.copies = {
            name: pltpu.make_async_copy(source, target, sems.at[i])
            for i, (name, source, target) in enumerate(zip(names, sources, targets))
        }

    def start(self):
        for copy in self.copies.values():
            copy.start()

    def wait(self, *names):
        for name in names:
            self.copies.pop(name).wait()


class View:
    def __init__(self, ref, base):
        self.ref = ref
        self.base = base

    def __getitem__(self, index):
        return self.ref[self.base + index]


def resolve_lists(packed, lists, first_row, result):
    for at in range(0, 32, 8):
        index = lists[at : at + 8, :]
        group = index >> 7
        lane = index & 127
        found = jnp.zeros((8, 128), jnp.int32)
        for row in range(packed.shape[0]):
            source = jnp.broadcast_to(packed[row : row + 1, :], (8, 128))
            taken = jnp.take_along_axis(source, lane, axis=1)
            found = jnp.where(group == row, taken, found)
        result[at : at + 8, :] = found & ((1 << PAIR_BITS) - 1)
        line = lax.broadcasted_iota(jnp.int32, (8, 128), 0) + at
        slot = lax.broadcasted_iota(jnp.int32, (8, 128), 1) + (line & 1) * 128
        here = (found >> PAIR_BITS) - 1 == first_row + (line >> 1)
        end = jnp.max(jnp.where(here, slot + 1, 0), axis=1, keepdims=True)
        result[32 + at : 40 + at, :] = jnp.broadcast_to(end, (8, 128))


def pack_rows(slots, info, pool, staging, outs, sems, capacity):
    copies = []
    for position, out in enumerate(outs):
        row = 2 * jnp.clip(info[0] + STEPS[position], 0, 2 * REACH)
        end = jnp.maximum(slots[32 + row, 0], slots[33 + row, 0])

        def chunk(k, carry, row=row, position=position):
            rows = []
            line = row + (k * PACK_UNROLL) // 128
            column = k * PACK_UNROLL % 128
            for u in range(PACK_UNROLL):
                rows.append(pool[pl.ds(slots[line, column + u], 1), :])
            for u in range(PACK_UNROLL):
                staging[pl.ds(position * capacity + k * PACK_UNROLL + u, 1), :] = rows[u]
            return carry

        lax.fori_loop(0, (end + PACK_UNROLL - 1) // PACK_UNROLL, chunk, 0)
        here = staging.at[position * capacity : (position + 1) * capacity, :]
        copies.append(pltpu.make_async_copy(here, out, sems.at[position]))
        copies[-1].start()
    for copy in copies:
        copy.wait()


FIRST_NAMES = ("traces",)
LAST_NAMES = ("off_main", "spread", "lift_main")


def first_kernel(elems, capacity):
    def body(*refs):
        start, size_ref, packed, lists, info = refs[:5]
        consts = dict(zip(FIRST_NAMES, refs[5 : 5 + len(FIRST_NAMES)]))
        x_out, pool, slots, *rest = refs[5 + len(FIRST_NAMES) :]
        outs = rest[: 2 * REACH]
        staging, out_sems, resolved, sem = rest[2 * REACH :]
        resolve_lists(packed, lists, info[1], resolved)
        copy = pltpu.make_async_copy(resolved, slots, sem)
        copy.start()
        x = jnp.concatenate([start[...].T, jnp.zeros((elems, 40), F32)], axis=1)
        x_out[...] = x
        write_tables(x, size_ref[...], consts, pool, elems)
        copy.wait()
        pack_rows(slots, info, pool, staging, outs, out_sems, capacity)

    return body


def compact_pairs(pairs, ranks, places, result, fill):
    lines = pairs.shape[0]
    flags = jnp.where(pairs[...] >= 0, 1.0, 0.0)
    columns = jnp.concatenate([flags, jnp.zeros((32 - lines, 128), F32)], axis=0).T.astype(BF)
    row = lax.broadcasted_iota(jnp.int32, (128, 128), 0)
    column = lax.broadcasted_iota(jnp.int32, (128, 128), 1)
    within = dot(jnp.where(row >= column, 1.0, 0.0).astype(BF), columns)
    earlier = jnp.where(row < column, 1.0, 0.0)[:32, :32].astype(BF)
    totals = jnp.broadcast_to(within[127:128, :], (8, 32)).astype(BF)
    before = dot(totals, earlier)[0:1, :]
    rank = within + before
    for line in range(lines):
        ranks[line * 128 : (line + 1) * 128, :] = jnp.broadcast_to(
            rank[:, line : line + 1], (128, 128)
        )
    count = jnp.sum(flags).astype(jnp.int32)
    places[...] = jnp.full(places.shape, float(lines * 128), F32)
    lane = lax.broadcasted_iota(jnp.int32, (8, 128), 1)

    def place(k, carry):
        target = (lane + k * 128).astype(F32)
        total = jnp.zeros((8, 128), F32)
        for at in range(0, lines * 128, 8):
            total = total + jnp.where(ranks[at : at + 8, :] <= target, 1.0, 0.0)
        places[pl.ds(k, 1), :] = jnp.sum(total, axis=0, keepdims=True)
        return carry

    lax.fori_loop(0, (count + 127) // 128, place, 0)
    for at in range(0, lines, 8):
        index = places[at : at + 8, :].astype(jnp.int32)
        found = jnp.full((8, 128), fill, jnp.int32)
        for line in range(lines):
            source = jnp.broadcast_to(pairs[line : line + 1, :], (8, 128))
            taken = jnp.take_along_axis(source, index & 127, axis=1)
            found = jnp.where((index >> 7) == line, taken, found)
        result[at : at + 8, :] = found
    return count


def add_rows(flag, count, source, target, pool, sums):
    @pl.when(flag == 0)
    def _():
        def chunk(k, carry):
            base = k * UNROLL
            rows = []
            for u in range(UNROLL):
                rows.append(pool[pl.ds(source(base, u), 1), :])
            for u in range(UNROLL):
                sums[pl.ds(target(base, u), 1), :] = rows[u]
            return carry

        lax.fori_loop(0, (count + UNROLL - 1) // UNROLL, chunk, 0)

    @pl.when(flag != 0)
    def _():
        def one(r, carry):
            here = pl.ds(target(r, 0), 1)
            sums[here, :] = sums[here, :] + pool[pl.ds(source(r, 0), 1), :]
            return carry

        lax.fori_loop(0, count, one, 0)


def inner_kernel(elems, records, compact):
    table_rows = 30 * elems

    def body(*refs):
        if compact:
            x_ref, size_ref, pool, ints, recs, far_pair, vol = refs[:7]
            sums, total, far_pairs, meta, counts_out, ranks, places, packed, sem = refs[7:]
            count = compact_pairs(far_pair, ranks, places, packed, table_rows)
            meta[0] = count
            copy = pltpu.make_async_copy(packed, far_pairs, sem)
            copy.start()
        else:
            x_ref, size_ref, pool, ints, meta, vol, sums, total = refs
        table_row, local_rec, local_row = (View(ints, i * records) for i in range(3))
        if compact:
            row_iota = lax.broadcasted_iota(jnp.int32, (64, records), 0)
            slabs = recs[1:2, :]
            weight = recs[2:3, :].astype(F32)
            low = jnp.where(row_iota == slabs, 1.0, 0.0)
            high = jnp.where(row_iota - 32 == slabs, 1.0, 0.0) * weight
            kinds = (low + high).astype(BF)
            elem_iota = lax.broadcasted_iota(jnp.int32, (elems, records), 0)
            onehot = jnp.where(elem_iota == recs[0:1, :], 1.0, 0.0).astype(BF)
            counts = lax.dot_general(
                onehot, kinds, (((1,), (1,)), ((), ())), preferred_element_type=F32
            )
            counts_out[...] = counts
            paired = 2.0 * counts[:, :32] - counts[:, 32:]
            flag = jnp.where(jnp.max(paired) > 1.5, 1, 0)
            meta[1] = flag
        else:
            flag = meta[1]

        def clear(k, carry):
            at = pl.multiple_of(k * elems, elems)
            sums[pl.ds(at, elems), :] = jnp.zeros((elems, 128), F32)
            return carry

        lax.fori_loop(0, 30, clear, 0)
        sums[table_rows : table_rows + 8, :] = jnp.zeros((8, 128), F32)
        add_rows(
            flag,
            records,
            lambda base, u: table_row[local_rec[base + u]],
            lambda base, u: local_row[base + u],
            pool,
            sums,
        )
        x_hi, x_lo = split(x_ref[...])
        hi = vol[:256, :]
        volume = dot(x_hi, hi) + dot(x_lo, hi) + dot(x_hi, vol[256:, :])
        size = size_ref[...]
        total[...] = volume * jnp.concatenate([size, size], axis=1)
        if compact:
            copy.wait()

    return body


def outer_kernel(elems, capacity, records, step, last):
    slab = 6 * elems
    table_rows = 5 * slab
    const_names = LAST_NAMES if last else LAST_NAMES + FIRST_NAMES
    block_names = tuple("block%d" % i for i in range(2 * REACH))

    def body(*refs):
        x_ref, dirn_ref, rhs_ref, size_ref, counts_ref, pool, near, volume, inv_diag = refs[:9]
        scalars, far_pairs, meta, slots, info = refs[9:14]
        received = refs[14 : 14 + 2 * REACH]
        at = 14 + 2 * REACH
        consts = dict(zip(const_names, refs[at : at + len(const_names)]))
        rest = refs[at + len(const_names) :]
        if last:
            earlier = rest[: ITERS - 1]
            sums, x_out, norm_out = rest[ITERS - 1 : ITERS + 2]
            rest = rest[ITERS + 2 :]
        else:
            sums, x_out, dirn_out, norm_out, pool = rest[:5]
            outs = rest[5 : 5 + 2 * REACH]
            rest = rest[5 + 2 * REACH :]
        blocks, total, sems, out_sems = rest
        fetch = Fetch(
            block_names,
            received,
            [blocks.at[i * capacity : (i + 1) * capacity, :] for i in range(2 * REACH)],
            sems,
        )
        fetch.start()
        size = size_ref[...]
        inverse = safe_inverse(size)
        fetch.wait(*block_names)
        add_rows(
            meta[1],
            meta[0],
            lambda base, u: far_pairs[base >> 7, (base & 127) + u] >> PAIR_BITS,
            lambda base, u: far_pairs[base >> 7, (base & 127) + u] & ((1 << PAIR_BITS) - 1),
            blocks,
            sums,
        )
        size_wide = jnp.concatenate([size, size], axis=1)
        total[...] = volume[...]
        counts = counts_ref[...].astype(BF)
        is_value, below_again = lane_groups(elems)

        def direction_terms(direction):
            at = pl.multiple_of(direction * elems, elems)
            acc = jnp.zeros((elems, 256), F32)
            spread = dot(counts, consts["spread"][direction])
            for sub in range(5):
                edge = size if sub == 4 else 0.5 * size
                area = -0.5 * edge * edge
                coef = jnp.where(is_value, edge, jnp.where(below_again, area, area * inverse))
                rows = pl.ds(sub * slab + at, elems)
                times = spread[:, sub * 128 : (sub + 1) * 128]
                term = coef * (pool[rows, :] * times - sums[rows, :])
                term_hi, term_lo = split(term)
                acc = acc + dot(
                    jnp.concatenate([term_hi, term_lo], axis=1), consts["off_main"][sub]
                )
            face = acc[:, :128] + acc[:, 128:]
            total[...] += dot(rows_of_three(face), consts["lift_main"][direction])

        each_direction(direction_terms)
        rhs = jnp.concatenate([rhs_ref[...].T, jnp.zeros((elems, 40), F32)], axis=1)
        residual = jnp.where(size_wide > 0.0, rhs - total[...], 0.0)
        scaled = residual * (jnp.concatenate([inverse, inverse], axis=1) * inv_diag[...])

        def fold(product):
            part = jnp.sum(product.reshape(elems // 8, 8, 256), axis=0)
            return part[:, :128] + part[:, 128:]

        folded = (fold(residual * residual), fold(residual * scaled))
        if last:
            pieces = [n[at : at + 8, :] for n in earlier for at in (0, 8)] + list(folded)
            lane = lax.broadcasted_iota(jnp.int32, norm_out.shape, 1)
            row = jnp.zeros(norm_out.shape, F32)
            for i, piece in enumerate(pieces):
                row = jnp.where(lane == i, jnp.sum(piece), row)
            norm_out[...] = row
        else:
            norm_out[0:8, :] = folded[0]
            norm_out[8:16, :] = folded[1]
        dirn = scalars[2 * step + 1] * scaled
        if step > 0:
            dirn = scalars[2 * step] * dirn_ref[...] + dirn
        x_new = x_ref[...] + dirn
        if last:
            x_out[...] = x_new[:, :216].T
        else:
            x_out[...] = x_new
            dirn_out[...] = dirn
            write_tables(x_new, size, consts, pool, elems)
            pack_rows(slots, info, pool, blocks, outs, out_sems, capacity)

    return body


def on_device(
    rhs, start, spectrum_top, elem_code, rec_elem, rec_dir, rec_sub, rec_peer, rec_index, send_rec
):
    consts = build_constants()
    parts = lax.axis_size(AXIS)
    own = lax.axis_index(AXIS)
    elems = rhs.shape[1]
    records = rec_elem.shape[0]
    capacity = send_rec.shape[0] // parts
    slab = 6 * elems
    table_rows = 5 * slab

    size = jnp.broadcast_to((0.5 * elem_code.astype(F32))[:, None], (elems, 128))
    sub = jnp.minimum(rec_sub, 4)
    table_row = sub * slab + rec_dir * elems + rec_elem
    live = rec_sub < 5
    bound = rec_peer < 0
    local = jnp.logical_and(rec_peer == own, live)
    far = jnp.logical_and(jnp.logical_not(bound), rec_peer != own)
    far = jnp.logical_and(far, live)
    offset = own - rec_peer
    position = jnp.where(offset > 0, offset - 1, 2 * REACH + offset)
    far_row = jnp.clip(position, 0, 2 * REACH - 1) * capacity + rec_index
    far_pair = jnp.where(far, far_row * (1 << PAIR_BITS) + table_row, -1)
    local_rec = jnp.where(local, rec_index, 0)
    local_row = jnp.where(local, table_row, table_rows)
    kind = jnp.where(live, sub * 6 + rec_dir, 99)
    recs = jnp.stack([rec_elem, kind, jnp.where(bound, 2, 1)])
    first_row = jnp.clip(own - REACH, 0, parts - 1 - 2 * REACH)
    lists = lax.dynamic_slice(
        send_rec.reshape(parts, capacity), (first_row, 0), (2 * REACH + 1, capacity)
    )
    lists = jnp.pad(lists.reshape(-1, 128), ((0, 2), (0, 0)))
    packed = ((rec_peer + 1) * (1 << PAIR_BITS) + table_row).reshape(-1, 128)
    info = jnp.stack([own - first_row, first_row]).astype(jnp.int32)

    top_value = spectrum_top[0]
    bottom = top_value / BOTTOM_RATIO
    center = 0.5 * (top_value + bottom)
    radius = 0.5 * (top_value - bottom)
    sigma_ratio = center / radius
    rho_prev = 1.0 / sigma_ratio
    factors = [jnp.zeros((), F32), 1.0 / center]
    for _ in range(1, ITERS):
        rho_next = 1.0 / (2.0 * sigma_ratio - rho_prev)
        factors += [rho_next * rho_prev, 2.0 * rho_next / radius]
        rho_prev = rho_next
    factors = jnp.stack(factors)
    near_ints = jnp.concatenate([table_row, local_rec, local_row])
    far_pair = far_pair.reshape(-1, 128)
    (size, packed, lists, info, near_ints, far_pair, recs, factors, start) = (
        lax.optimization_barrier(
            (size, packed, lists, info, near_ints, far_pair, recs, factors, start)
        )
    )

    vmem = pl.BlockSpec(memory_space=pltpu.VMEM)
    smem = pl.BlockSpec(memory_space=pltpu.SMEM)
    hbm = pl.BlockSpec(memory_space=pltpu.HBM)
    field = jax.ShapeDtypeStruct((elems, 256), F32)
    block = jax.ShapeDtypeStruct((capacity, 128), F32)
    table = jax.ShapeDtypeStruct((table_rows, 128), F32)
    table_more = jax.ShapeDtypeStruct((table_rows + 8, 128), F32)
    params = pltpu.CompilerParams(vmem_limit_bytes=VMEM_MIB << 20)
    small = pltpu.CompilerParams(vmem_limit_bytes=SMALL_MIB << 20)
    staging = pltpu.VMEM((2 * REACH * capacity, 128), F32)
    blocks_out = (block,) * (2 * REACH)
    nodes = rhs.shape[0]

    def pick(names):
        return [consts[n] for n in names]

    def sems(count):
        return pltpu.SemaphoreType.DMA((count,))

    x, pool, slots, *blocks = pl.pallas_call(
        first_kernel(elems, capacity),
        name="first_traces",
        out_shape=(field, table, jax.ShapeDtypeStruct((64, 128), jnp.int32)) + blocks_out,
        in_specs=[vmem] * 4 + [smem] + [vmem] * len(FIRST_NAMES),
        out_specs=(vmem, vmem, smem) + (hbm,) * (2 * REACH),
        scratch_shapes=[
            staging,
            sems(2 * REACH),
            pltpu.VMEM((64, 128), jnp.int32),
            pltpu.SemaphoreType.DMA,
        ],
        compiler_params=small,
    )(start, size, packed, lists, info, *pick(FIRST_NAMES))

    dirn = x
    norms = []
    for step in range(ITERS):
        last = step == ITERS - 1
        compact = step == 0
        received = [
            lax.ppermute(piece, AXIS, [(i, (i + by) % parts) for i in range(parts)])
            for piece, by in zip(blocks, STEPS)
        ]
        lines = records // 128
        pair_lines = jax.ShapeDtypeStruct((lines, 128), jnp.int32)
        results = pl.pallas_call(
            inner_kernel(elems, records, compact),
            name="inner_%d" % step,
            out_shape=(table_more, field)
            + (
                (
                    pair_lines,
                    jax.ShapeDtypeStruct((2,), jnp.int32),
                    jax.ShapeDtypeStruct((elems, 64), F32),
                )
                if compact
                else ()
            ),
            in_specs=[vmem] * 3 + [smem] + ([vmem, vmem] if compact else [smem]) + [vmem],
            out_specs=(vmem, vmem) + ((smem, smem, vmem) if compact else ()),
            scratch_shapes=[
                pltpu.VMEM((records, 128), F32),
                pltpu.VMEM((lines, 128), F32),
                pltpu.VMEM((lines, 128), jnp.int32),
                pltpu.SemaphoreType.DMA,
            ]
            if compact
            else [],
            compiler_params=small,
            cost_estimate=pl.CostEstimate(
                flops=10**10, transcendentals=0, bytes_accessed=10**6
            ),
        )(
            x,
            size,
            pool,
            near_ints,
            *((recs, far_pair) if compact else (meta,)),
            consts["volume"],
        )
        near, volume = results[:2]
        if compact:
            far_list, meta, counts = results[2:]
        norm_shape = jax.ShapeDtypeStruct((16, 128), F32)
        if last:
            shapes = (
                table_more,
                jax.ShapeDtypeStruct((nodes, elems), F32),
                jax.ShapeDtypeStruct((parts, 128), F32),
            )
            out_specs = (vmem,) * 3
        else:
            shapes = (table_more, field, field, norm_shape, table) + blocks_out
            out_specs = (vmem,) * 5 + (hbm,) * (2 * REACH)
        names = LAST_NAMES if last else LAST_NAMES + FIRST_NAMES
        results = pl.pallas_call(
            outer_kernel(elems, capacity, records, step, last),
            name="outer_%d" % step,
            out_shape=shapes,
            in_specs=[vmem] * 9
            + [smem] * 5
            + [hbm] * (2 * REACH)
            + [vmem] * (len(names) + (len(norms) if last else 0)),
            out_specs=out_specs,
            scratch_shapes=[
                staging,
                pltpu.VMEM((elems, 256), F32),
                sems(2 * REACH),
                sems(2 * REACH),
            ],
            input_output_aliases={6: 0} if last else {6: 0, 5: 4},
            compiler_params=params,
        )(
            x,
            dirn,
            rhs,
            size,
            counts,
            pool,
            near,
            volume,
            consts["inv_diag"],
            factors,
            far_list,
            meta,
            slots,
            info,
            *received,
            *pick(names),
            *(norms if last else ()),
        )
        if last:
            _, answer, mine = results
        else:
            _, x, dirn, norm, pool, *blocks = results
            norms.append(norm)

    gathered = lax.all_to_all(mine, AXIS, 0, 0, tiled=True)
    total = jnp.sum(gathered, axis=0)[:6].reshape(3, 2)
    return (answer, 0.5 * jnp.log(total / (216.0 * elems * parts)))


def solution(mesh):
    split_spec = P(AXIS)
    in_specs = (P(None, AXIS), P(None, AXIS), P()) + (split_spec,) * 7
    out_specs = (P(None, AXIS), P())
    return jax.shard_map(
        on_device, mesh=mesh, in_specs=in_specs, out_specs=out_specs, check_vma=False
    )
```
